64 devices in a mesh: dp: 4 (over x, y), tp: 16 (over z, core).
Axes of the slice: x: 2, y: 2, z: 8, core: 2. Of those that a mesh axis runs over, the one named last changes fastest.
The devices are a block of a 4x4x8 slice.
Arguments:
- token_ids: int32 [65536], P('dp'), parts along dimension 0
- embed_table: bfloat16 [152064, 128], P('tp')
- norm_gain: bfloat16 [128], replicated
- w_up: bfloat16 [128, 18944], P(None, 'tp')
- w_down: bfloat16 [18944, 128], P('tp')
- d_out: bfloat16 [65536, 128], P(('dp', 'tp')), parts along dimension 0
Outputs:
- output 1: bfloat16 [65536, 128], P(('dp', 'tp')), parts along dimension 0
- output 2: float32 [608256, 128], P(('dp', 'tp')), parts along dimension 0
- output 3: float32 [512, 18944], P('dp', 'tp'), parts along dimension 0
- output 4: float32 [75776, 128], P(('dp', 'tp')), parts along dimension 0
There are 4 independent parts. The reference program is written for one: setup_inputs(seed, part) draws one part's arguments, and reference() takes and returns one part's arrays. A program takes and returns all parts, laid end to end along the dimension named above; an argument that names none is the same for every part.
All inputs are finite; a program needn't handle non-finite values.
Results may differ from the reference program's by a relative error of at most 0.00933744.
Values are sent between devices in bfloat16 or wider.
A program may use at most 768 MiB of HBM per device.

```python
import math
import jax
import jax.numpy as jnp
from jax import lax

TOKENS = 16384
VOCAB_SIZE = 152064
MODEL_DIM = 128
HIDDEN = 18944
POOL_SIZE = TOKENS // 2
ROW_BLOCK = math.gcd(TOKENS, 512)
NORM_EPS = 1e-6


def gelu_tanh(values):
    return jax.nn.gelu(values, approximate=True)


def draw_ids(pool_key, pick_key, perm_key):
    pool_ids = jax.random.randint(pool_key, (POOL_SIZE,), 0, VOCAB_SIZE, dtype=jnp.int32)
    pool_ids = pool_ids.at[0].set(0).at[1].set(VOCAB_SIZE - 1)
    picks = jax.random.randint(pick_key, (TOKENS - POOL_SIZE,), 0, POOL_SIZE, dtype=jnp.int32)
    token_ids = jnp.concatenate([pool_ids, pool_ids[picks]])
    return jax.random.permutation(perm_key, token_ids)


def setup_inputs(seed: int = 0, part: int = 0) -> dict:
    base_key = jax.random.key(seed)
    k_table, k_gain, k_up, k_down, k_part = jax.random.split(base_key, 5)
    part_key = jax.random.fold_in(k_part, part)
    k_pool, k_pick, k_perm, k_grad = jax.random.split(part_key, 4)
    embed_table = jax.random.normal(k_table, (VOCAB_SIZE, MODEL_DIM), jnp.float32)
    norm_gain = 0.5 + jax.random.uniform(k_gain, (MODEL_DIM,), jnp.float32)
    w_up = jax.random.normal(k_up, (MODEL_DIM, HIDDEN), jnp.float32) * MODEL_DIM ** -0.5
    w_down = jax.random.normal(k_down, (HIDDEN, MODEL_DIM), jnp.float32) * HIDDEN ** -0.5
    d_out = jax.random.normal(k_grad, (TOKENS, MODEL_DIM), jnp.float32)
    return {
        "token_ids": draw_ids(k_pool, k_pick, k_perm),
        "embed_table": embed_table.astype(jnp.bfloat16),
        "norm_gain": norm_gain.astype(jnp.bfloat16),
        "w_up": w_up.astype(jnp.bfloat16),
        "w_down": w_down.astype(jnp.bfloat16),
        "d_out": d_out.astype(jnp.bfloat16),
    }


def reference(token_ids, embed_table, norm_gain, w_up, w_down, d_out):
    gain_f32 = norm_gain.astype(jnp.float32)
    num_blocks = TOKENS // ROW_BLOCK
    embed_blocks = embed_table[token_ids].reshape(num_blocks, ROW_BLOCK, MODEL_DIM)
    grad_blocks = d_out.reshape(num_blocks, ROW_BLOCK, MODEL_DIM)

    def block_step(grad_acc, block_in):
        acc_up, acc_down = grad_acc
        embed_rows, grad_rows = block_in
        embed_f32 = embed_rows.astype(jnp.float32)
        inv_rms = lax.rsqrt(jnp.mean(embed_f32 * embed_f32, axis=-1, keepdims=True) + NORM_EPS)
        normed = (embed_f32 * inv_rms * gain_f32).astype(jnp.bfloat16)
        up_act = jnp.dot(normed, w_up, preferred_element_type=jnp.float32).astype(jnp.bfloat16)
        hid_f32, gelu_vjp = jax.vjp(gelu_tanh, up_act.astype(jnp.float32))
        hid_act = hid_f32.astype(jnp.bfloat16)
        mlp_out = jnp.dot(hid_act, w_down, preferred_element_type=jnp.float32)
        block_out = (embed_f32 + mlp_out).astype(jnp.bfloat16)
        d_hid = jnp.dot(grad_rows, w_down.T, preferred_element_type=jnp.float32)
        d_up_act = gelu_vjp(d_hid)[0].astype(jnp.bfloat16)
        acc_down = acc_down + jnp.dot(hid_act.T, grad_rows, preferred_element_type=jnp.float32)
        acc_up = acc_up + jnp.dot(normed.T, d_up_act, preferred_element_type=jnp.float32)
        d_norm = jnp.dot(d_up_act, w_up.T, preferred_element_type=jnp.float32)
        d_scaled = d_norm * gain_f32
        mean_term = jnp.mean(embed_f32 * d_scaled, axis=-1, keepdims=True)
        d_embed = inv_rms * (d_scaled - embed_f32 * inv_rms * inv_rms * mean_term)
        d_embed = (grad_rows.astype(jnp.float32) + d_embed).astype(jnp.bfloat16)
        return (acc_up, acc_down), (block_out, d_embed)

    zero_grads = (jnp.zeros((MODEL_DIM, HIDDEN), jnp.float32), jnp.zeros((HIDDEN, MODEL_DIM), jnp.float32))
    (grad_up, grad_down), (out_blocks, d_embed_blocks) = lax.scan(block_step, zero_grads, (embed_blocks, grad_blocks))
    block_out = out_blocks.reshape(TOKENS, MODEL_DIM)
    d_embed = d_embed_blocks.reshape(TOKENS, MODEL_DIM).astype(jnp.float32)
    grad_table = jax.ops.segment_sum(d_embed, token_ids, num_segments=VOCAB_SIZE)
    return block_out, grad_table, grad_up, grad_down
```

```python
import functools

import jax
import jax.numpy as jnp
from jax import lax
from jax.experimental import pallas as pl
from jax.experimental.pallas import tpu as pltpu
from jax.sharding import PartitionSpec as P

NORM_EPS = 1e-6
GELU_C = 0.7978845608028654
GELU_A = 0.044715
MESH = pl.DeviceIdType.MESH
F32 = jnp.float32
BF16 = jnp.bfloat16


def remote(src, dst, send_sem, recv_sem, dev):
    return pltpu.make_async_remote_copy(
        src_ref=src, dst_ref=dst, send_sem=send_sem, recv_sem=recv_sem,
        device_id={"tp": dev}, device_id_type=MESH,
    )


def block_kernel(
    chips, sub,
    idx_ref, table_ref, gain_ref, w1_ref, w1t_ref, w2_ref, w2t_ref, dout_ref,
    out_ref, dw1t_ref, dw2_ref, dx_all,
    tab_in, tab_f32, gath, xs, x_t, inv_r, d_all, n_all, h_buf, du_buf, own, psend, precv, rs,
    tab_sem, x_send, x_recv, d_send, d_recv, dp_send, dp_recv, n_send, n_recv, np_send, np_recv,
    e_send, e_recv, ep_send, ep_recv, p_send, p_recv, r_send, r_recv,
):
    me = lax.axis_index("tp")
    chip, core = me // 2, me % 2
    partner = chip * 2 + 1 - core
    up = ((chip + 1) % chips) * 2 + core
    down = ((chip + chips - 1) % chips) * 2 + core
    half_rows = gath.shape[1]
    shard_rows = table_ref.shape[0]
    steps = chips - 1

    def next_dev(half):
        return up * (1 - half) + down * half

    def chip_at(half, hop):
        return (chip + (1 - half) * (chips - hop) + half * hop) % chips

    barrier = pltpu.get_barrier_semaphore()
    for dev in (partner, up, down):
        pl.semaphore_signal(barrier, inc=1, device_id={"tp": dev}, device_id_type=MESH)
    pl.semaphore_wait(barrier, 3)

    def ring_copy(buf, send, recv, half, step):
        blk = chip_at(half, step) * 2 + core
        return remote(buf.at[half, blk], buf.at[half, blk], send.at[half, step], recv.at[half, step], next_dev(half))

    def ring_arrival(buf, send, recv, half, step):
        blk = chip_at(half, step + 1) * 2 + core
        return remote(buf.at[half, blk], buf.at[half, blk], send.at[half, step], recv.at[half, step], next_dev(half))

    def pair_copy(buf, send, recv, half, hop):
        blk = chip_at(half, hop) * 2 + core
        return remote(buf.at[half, blk], buf.at[half, blk], send.at[half, hop], recv.at[half, hop], partner)

    def pair_arrival(buf, send, recv, half, hop):
        blk = chip_at(half, hop) * 2 + 1 - core
        return remote(buf.at[half, blk], buf.at[half, blk], send.at[half, hop], recv.at[half, hop], partner)

    def gather_begin(buf, sems, half):
        send, recv, psend_, precv_ = sems
        ring_copy(buf, send, recv, half, 0).start()
        pair_copy(buf, psend_, precv_, half, 0).start()

    def gather_step(buf, sems, half, step):
        send, recv, psend_, precv_ = sems
        ring_arrival(buf, send, recv, half, step).wait_recv()

        @pl.when(step + 1 < steps)
        def _():
            ring_copy(buf, send, recv, half, step + 1).start()

        pair_copy(buf, psend_, precv_, half, step + 1).start()

    def gather_drain(buf, sems):
        send, recv, psend_, precv_ = sems

        def body(step, _):
            for half in (0, 1):
                ring_copy(buf, send, recv, half, step).wait_send()
            return 0

        lax.fori_loop(0, steps, body, 0)

        def pair_body(hop, _):
            for half in (0, 1):
                pair_copy(buf, psend_, precv_, half, hop).wait_send()
            return 0

        lax.fori_loop(0, chips, pair_body, 0)

    d_sems = (d_send, d_recv, dp_send, dp_recv)
    n_sems = (n_send, n_recv, np_send, np_recv)
    e_sems = (e_send, e_recv, ep_send, ep_recv)

    tab_copy = remote(table_ref, tab_in, tab_sem.at[0], tab_sem.at[1], partner)
    tab_copy.start()
    for half in (0, 1):
        rows = dout_ref[half * half_rows:(half + 1) * half_rows, :].astype(F32)
        d_all[half, me] = rows.T.astype(BF16)
        gather_begin(d_all, d_sems, half)
    dw1t_ref[...] = jnp.zeros(dw1t_ref.shape, F32)
    dw2_ref[...] = jnp.zeros(dw2_ref.shape, F32)
    conv = 32

    def convert(src, start):
        def body(i, _):
            at = pl.multiple_of(i * conv, conv)
            dst = pl.multiple_of(start + i * conv, conv)
            tab_f32[pl.ds(dst, conv), :] = src[pl.ds(at, conv), :].astype(F32)
            return 0

        lax.fori_loop(0, shard_rows // conv, body, 0)

    convert(table_ref, core * shard_rows)
    tab_f32[pl.ds(2 * shard_rows, 8), :] = jnp.zeros((8, tab_f32.shape[1]), F32)
    tab_copy.wait()
    convert(tab_in, (1 - core) * shard_rows)

    def x_copy(half, step):
        return remote(xs.at[half, step], xs.at[half, step + 1], x_send.at[half, step], x_recv.at[half, step],
                      next_dev(half))

    unroll = 8

    def look_step(step, _):
        for half in (0, 1):
            base = (chip_at(half, step + 1) * 2 + half) * half_rows

            def rows_body(i, _):
                at = i * unroll
                for j in range(unroll):
                    row = idx_ref[base + at + j]
                    gath[half, pl.ds(at + j, 1), :] = tab_f32[pl.ds(row, 1), :]
                return 0

            lax.fori_loop(0, half_rows // unroll, rows_body, 0)

            @pl.when(step == 0)
            def _():
                xs[half, step] = gath[half].astype(BF16)

            @pl.when(step > 0)
            def _():
                x_copy(half, step - 1).wait_recv()
                xs[half, step] = (gath[half] + xs[half, step].astype(F32)).astype(BF16)

            @pl.when(step < steps)
            def _():
                x_copy(half, step).start()

        @pl.when(step < steps)
        def _():
            for half in (0, 1):
                gather_step(d_all, d_sems, half, step)

        return 0

    lax.fori_loop(0, chips, look_step, 0)

    gain = gain_ref[...]
    for half in (0, 1):
        rows_t = xs[half, steps].astype(F32).T
        inv = lax.rsqrt(jnp.mean(rows_t * rows_t, axis=0, keepdims=True) + NORM_EPS)
        x_t[half] = rows_t
        inv_r[half] = inv
        n_all[half, me] = (rows_t * inv * gain).astype(BF16)
        gather_begin(n_all, n_sems, half)

    def d_wait(hop, _):
        for half in (0, 1):
            pair_arrival(d_all, dp_send, dp_recv, half, hop).wait_recv()
        return 0

    lax.fori_loop(0, chips, d_wait, 0)

    def mlp(half, blk, dst):
        def body(i, _):
            cols = pl.ds(pl.multiple_of(i * sub, sub), sub)
            n_t = n_all[half, blk, :, cols]
            d_t = d_all[half, blk, :, cols]
            u = jnp.dot(w1t_ref[...], n_t, preferred_element_type=F32).astype(BF16).astype(F32)
            dh = jnp.dot(w2_ref[...], d_t, preferred_element_type=F32)
            sq = u * u
            th = jnp.tanh(u * (GELU_C + (GELU_C * GELU_A) * sq))
            sg = 0.5 + 0.5 * th
            h = u * sg
            slope = sg + (h * (1.0 - sg)) * (2.0 * GELU_C + (6.0 * GELU_C * GELU_A) * sq)
            h = h.astype(BF16)
            du = (dh * slope).astype(BF16)
            h_buf[...] = h
            du_buf[...] = du
            h = h_buf[...]
            du = du_buf[...]
            dst[0, :, cols] = jnp.dot(w2t_ref[...], h, preferred_element_type=F32)
            dst[1, :, cols] = jnp.dot(w1_ref[...], du, preferred_element_type=F32)
            nt = (((1,), (1,)), ((), ()))
            dw2_ref[...] += lax.dot_general(h, d_t, nt, preferred_element_type=F32)
            dw1t_ref[...] += lax.dot_general(du, n_t, nt, preferred_element_type=F32)
            return 0

        lax.fori_loop(0, half_rows // sub, body, 0)

    def p_copy(half, step):
        return remote(psend.at[step % 2, half], precv.at[step, half], p_send.at[step, half], p_recv.at[step, half],
                      partner)

    def r_copy(half, val, step):
        return remote(rs.at[step, half, val], rs.at[step + 1, half, val], r_send.at[step, half, val],
                      r_recv.at[step, half, val], next_dev(half))

    for half in (0, 1):
        gather_step(n_all, n_sems, half, 0)

    def sum_step(step, _):
        hop = (step + 1) % chips

        def part(i, _):
            half, mine = i % 2, i // 2
            blk = chip_at(half, hop) * 2 + (1 - core) * (1 - mine) + core * mine

            @pl.when(mine == 0)
            def _():
                pair_arrival(n_all, np_send, np_recv, half, hop).wait_recv()

                @pl.when(step >= 2)
                def _():
                    p_copy(half, step - 2).wait_send()

            @pl.when((i == 2) & (step + 1 < steps))
            def _():
                for h in (0, 1):
                    gather_step(n_all, n_sems, h, step + 1)

            mlp(half, blk, own.at[i])

            @pl.when(mine == 0)
            def _():
                psend[step % 2, half] = own[i]
                p_copy(half, step).start()

            @pl.when(mine == 1)
            def _():
                p_copy(half, step).wait_recv()
                for val in (0, 1):
                    @pl.when(step == 0)
                    def _():
                        rs[step, half, val] = own[i, val] + precv[step, half, val]

                    @pl.when(step > 0)
                    def _():
                        r_copy(half, val, step - 1).wait_recv()
                        rs[step, half, val] = rs[step, half, val] + (own[i, val] + precv[step, half, val])

                    @pl.when(step < steps)
                    def _():
                        r_copy(half, val, step).start()

            return 0

        lax.fori_loop(0, 4, part, 0)
        return 0

    lax.fori_loop(0, chips, sum_step, 0)

    for half in (0, 1):
        xv = x_t[half]
        inv = inv_r[half]
        rows = slice(half * half_rows, (half + 1) * half_rows)
        scaled = rs[steps, half, 1] * gain
        mean = jnp.mean(xv * scaled, axis=0, keepdims=True)
        dx = inv * (scaled - xv * inv * inv * mean)
        dx = dout_ref[rows, :].astype(F32) + dx.T
        dx_all[half, me] = dx.astype(BF16)
        gather_begin(dx_all, e_sems, half)
    for half in (0, 1):
        rows = slice(half * half_rows, (half + 1) * half_rows)
        out_ref[rows, :] = (x_t[half] + rs[steps, half, 0]).T.astype(BF16)

    def e_step(step, _):
        for half in (0, 1):
            gather_step(dx_all, e_sems, half, step)
        return 0

    lax.fori_loop(0, steps, e_step, 0)

    def e_wait(hop, _):
        for half in (0, 1):
            pair_arrival(dx_all, ep_send, ep_recv, half, hop).wait_recv()
        return 0

    lax.fori_loop(0, chips, e_wait, 0)

    for buf, sems in ((d_all, d_sems), (n_all, n_sems), (dx_all, e_sems)):
        gather_drain(buf, sems)

    def drain(step, _):
        for half in (0, 1):
            x_copy(half, step).wait_send()
            for val in (0, 1):
                r_copy(half, val, step).wait_send()
        return 0

    lax.fori_loop(0, steps, drain, 0)
    for half in (0, 1):
        for step in (chips - 2, chips - 1):
            p_copy(half, step).wait_send()


def run_block(chips, idx, table, gain, w_up, w_down, d_out):
    rows, dim = d_out.shape
    shard_rows = table.shape[0]
    hidden = w_down.shape[0]
    half = rows // 2
    devs = 2 * chips
    sub = min(256, half)
    dma = pltpu.SemaphoreType.DMA
    vmem = pl.BlockSpec(memory_space=pltpu.VMEM)
    w_up_t, w_down_t = w_up.T, w_down.T
    tokens = rows * devs
    return pl.pallas_call(
        functools.partial(block_kernel, chips, sub),
        out_shape=(
            jax.ShapeDtypeStruct((rows, dim), BF16),
            jax.ShapeDtypeStruct((hidden, dim), F32),
            jax.ShapeDtypeStruct((hidden, dim), F32),
            jax.ShapeDtypeStruct((2, devs, half, dim), BF16),
        ),
        in_specs=[pl.BlockSpec(memory_space=pltpu.SMEM)] + [vmem] * 7,
        out_specs=(vmem,) * 4,
        scratch_shapes=[
            pltpu.VMEM((shard_rows, dim), BF16),
            pltpu.VMEM((2 * shard_rows + 8, dim), F32),
            pltpu.VMEM((2, half, dim), F32),
            pltpu.VMEM((2, chips, half, dim), BF16),
            pltpu.VMEM((2, dim, half), F32),
            pltpu.VMEM((2, 1, half), F32),
            pltpu.VMEM((2, devs, dim, half), BF16),
            pltpu.VMEM((2, devs, dim, half), BF16),
            pltpu.VMEM((hidden, sub), BF16),
            pltpu.VMEM((hidden, sub), BF16),
            pltpu.VMEM((4, 2, dim, half), F32),
            pltpu.VMEM((2, 2, 2, dim, half), F32),
            pltpu.VMEM((chips, 2, 2, dim, half), F32),
            pltpu.VMEM((chips, 2, 2, dim, half), F32),
            dma((2,)),
            dma((2, chips - 1)), dma((2, chips - 1)),
            dma((2, chips - 1)), dma((2, chips - 1)), dma((2, chips)), dma((2, chips)),
            dma((2, chips - 1)), dma((2, chips - 1)), dma((2, chips)), dma((2, chips)),
            dma((2, chips - 1)), dma((2, chips - 1)), dma((2, chips)), dma((2, chips)),
            dma((chips, 2)), dma((chips, 2)),
            dma((chips - 1, 2, 2)), dma((chips - 1, 2, 2)),
        ],
        compiler_params=pltpu.CompilerParams(
            collective_id=0, has_side_effects=True, vmem_limit_bytes=67043328,
        ),
        cost_estimate=pl.CostEstimate(flops=12 * tokens * hidden * dim, bytes_accessed=tokens * dim * 8,
                                      transcendentals=0),
        name="block",
    )(idx, table, gain, w_up, w_up_t, w_down, w_down_t, d_out)


def scatter_kernel(rel_ref, words_ref, dx_ref, grad_ref, dx_f32):
    grad_ref[...] = jnp.zeros(grad_ref.shape, F32)
    conv = 128

    def convert(i, _):
        at = pl.multiple_of(i * conv, conv)
        dx_f32[pl.ds(at, conv), :] = dx_ref[pl.ds(at, conv), :].astype(F32)
        return 0

    lax.fori_loop(0, dx_ref.shape[0] // conv, convert, 0)

    def word_body(w, _):
        def cond(bits):
            return bits != 0

        def step(bits):
            low = bits & (-bits)
            tok = w * 32 + 31 - lax.clz(low)
            row = rel_ref[tok]
            grad_ref[pl.ds(row, 1), :] += dx_f32[pl.ds(tok, 1), :]
            return bits & (bits - 1)

        lax.while_loop(cond, step, words_ref[w])
        return 0

    lax.fori_loop(0, words_ref.shape[0], word_body, 0)


def scatter_rows(ids, base, shard_rows, dx_all):
    tokens, dim = dx_all.shape
    rel = ids - base
    owned = (rel >= 0) & (rel < shard_rows)
    bit = jnp.left_shift(jnp.int32(1), lax.broadcasted_iota(jnp.int32, (tokens // 32, 32), 1))
    words = jnp.sum(jnp.where(owned.reshape(tokens // 32, 32), bit, 0), axis=1, dtype=jnp.int32)
    smem = pl.BlockSpec(memory_space=pltpu.SMEM)
    vmem = pl.BlockSpec(memory_space=pltpu.VMEM)
    return pl.pallas_call(
        scatter_kernel,
        out_shape=jax.ShapeDtypeStruct((shard_rows, dim), F32),
        in_specs=[smem, smem, vmem],
        out_specs=vmem,
        scratch_shapes=[pltpu.VMEM((tokens, dim), F32)],
        compiler_params=pltpu.CompilerParams(vmem_limit_bytes=40 * 1024 * 1024),
        name="scatter",
    )(rel, words, dx_all)


def solution(mesh):
    chips = mesh.shape["tp"] // 2

    def shard_body(token_ids, embed_table, norm_gain, w_up, w_down, d_out):
        shard_rows, dim = embed_table.shape
        rows = d_out.shape[0]
        me = lax.axis_index("tp")
        chip, core = me // 2, me % 2
        rel = token_ids - chip * (2 * shard_rows)
        idx = jnp.where((rel >= 0) & (rel < 2 * shard_rows), rel, 2 * shard_rows)
        idx = lax.dynamic_index_in_dim(idx.reshape(chips, 2, rows), core, 1, keepdims=False).reshape(-1)
        gain = jnp.broadcast_to(norm_gain.astype(F32)[:, None], (dim, rows // 2))
        block_out, dw1t, dw2, dx_all = run_block(chips, idx, embed_table, gain, w_up, w_down, d_out)
        ids = token_ids.reshape(2 * chips, 2, rows // 2).transpose(1, 0, 2).reshape(-1)
        grad_table = scatter_rows(ids, me * shard_rows, shard_rows, dx_all.reshape(-1, dim))
        return block_out, grad_table, dw1t.T, dw2

    return jax.shard_map(
        shard_body,
        mesh=mesh,
        in_specs=(P("dp"), P("tp", None), P(), P(None, "tp"), P("tp", None), P(("dp", "tp"), None)),
        out_specs=(P(("dp", "tp"), None), P(("dp", "tp"), None), P("dp", "tp"), P(("dp", "tp"), None)),
        check_vma=False,
    )
```

```python
import functools

import jax
import jax.numpy as jnp
from jax import lax
from jax.experimental import pallas as pl
from jax.experimental.pallas import tpu as pltpu
from jax.sharding import PartitionSpec as P

NORM_EPS = 1e-6
GELU_C = 0.7978845608028654
GELU_A = 0.044715
MESH = pl.DeviceIdType.MESH
F32 = jnp.float32
BF16 = jnp.bfloat16


def remote(src, dst, send_sem, recv_sem, dev):
    return pltpu.make_async_remote_copy(
        src_ref=src, dst_ref=dst, send_sem=send_sem, recv_sem=recv_sem,
        device_id={"tp": dev}, device_id_type=MESH,
    )


def block_kernel(
    chips, sub, tiles,
    ids_ref, ids_vec, table_ref, gain_ref, w1t_ref, w2_ref, dout_ref,
    out_ref, dw1t_ref, dw2_ref, dx_all, list_ref, count_ref,
    tab_in, tab_f32, gath, xs, x_t, inv_r, gain_t, w1_ref, w2t_ref, d_all, n_all, h_buf, du_buf, parts, precv, rs,
    tab_sem, x_send, x_recv, d_send, d_recv, dp_send, dp_recv, n_send, n_recv, np_send, np_recv,
    e_send, e_recv, ep_send, ep_recv, p_send, p_recv, r_send, r_recv,
):
    me = lax.axis_index("tp")
    chip, core = me // 2, me % 2
    partner = chip * 2 + 1 - core
    up = ((chip + 1) % chips) * 2 + core
    down = ((chip + chips - 1) % chips) * 2 + core
    half_rows, dim = gath.shape[1:]
    shard_rows = table_ref.shape[0]
    steps = chips - 1

    def next_dev(half):
        return up * (1 - half) + down * half

    def chip_at(half, hop):
        return (chip + (1 - half) * (chips - hop) + half * hop) % chips

    barrier = pltpu.get_barrier_semaphore()
    for dev in (partner, up, down):
        pl.semaphore_signal(barrier, inc=1, device_id={"tp": dev}, device_id_type=MESH)
    pl.semaphore_wait(barrier, 3)

    def ring_copy(buf, send, recv, half, hop, step, piece):
        blk = chip_at(half, hop) * 2 + core
        pieces = send.shape[2]
        size = buf.shape[2] // pieces
        ref = buf.at[half, blk, pl.ds(piece * size, size)]
        return remote(ref, ref, send.at[half, step, piece], recv.at[half, step, piece], next_dev(half))

    def pair_copy(buf, send, recv, half, hop):
        blk = chip_at(half, hop) * 2 + core
        return remote(buf.at[half, blk], buf.at[half, blk], send.at[half, hop], recv.at[half, hop], partner)

    def pair_arrival(buf, send, recv, half, hop):
        blk = chip_at(half, hop) * 2 + 1 - core
        return remote(buf.at[half, blk], buf.at[half, blk], send.at[half, hop], recv.at[half, hop], partner)

    def gather_begin(buf, sems, half):
        send, recv, psend_, precv_ = sems
        for piece in range(send.shape[2]):
            ring_copy(buf, send, recv, half, 0, 0, piece).start()
        pair_copy(buf, psend_, precv_, half, 0).start()

    def gather_step(buf, sems, step):
        send, recv, psend_, precv_ = sems
        for piece in range(send.shape[2]):
            for half in (0, 1):
                ring_copy(buf, send, recv, half, step + 1, step, piece).wait_recv()

                @pl.when(step + 1 < steps)
                def _():
                    ring_copy(buf, send, recv, half, step + 1, step + 1, piece).start()

        for half in (0, 1):
            pair_copy(buf, psend_, precv_, half, step + 1).start()

    def gather_drain(buf, sems):
        send, recv, psend_, precv_ = sems

        def body(step, _):
            for half in (0, 1):
                for piece in range(send.shape[2]):
                    ring_copy(buf, send, recv, half, step, step, piece).wait_send()
            return 0

        lax.fori_loop(0, steps, body, 0)

        def pair_body(hop, _):
            for half in (0, 1):
                pair_copy(buf, psend_, precv_, half, hop).wait_send()
            return 0

        lax.fori_loop(0, chips, pair_body, 0)

    d_sems = (d_send, d_recv, dp_send, dp_recv)
    n_sems = (n_send, n_recv, np_send, np_recv)
    e_sems = (e_send, e_recv, ep_send, ep_recv)

    tab_copy = remote(table_ref, tab_in, tab_sem.at[0], tab_sem.at[1], partner)
    tab_copy.start()
    for half in (0, 1):
        rows = dout_ref[half * half_rows:(half + 1) * half_rows, :].astype(F32)
        d_all[half, me] = rows.T.astype(BF16)
        gather_begin(d_all, d_sems, half)
    conv = 32

    def convert(src, start):
        def body(i, _):
            at = pl.multiple_of(i * conv, conv)
            dst = pl.multiple_of(start + i * conv, conv)
            tab_f32[pl.ds(dst, conv), :] = src[pl.ds(at, conv), :].astype(F32)
            return 0

        lax.fori_loop(0, shard_rows // conv, body, 0)

    convert(table_ref, core * shard_rows)
    tab_f32[pl.ds(2 * shard_rows, 8), :] = jnp.zeros((8, dim), F32)
    tab_copy.wait()
    convert(tab_in, (1 - core) * shard_rows)

    pieces = x_send.shape[2]
    size = half_rows // pieces

    def x_copy(half, step, piece):
        rows = pl.ds(piece * size, size)
        return remote(xs.at[half, step, rows], xs.at[half, step + 1, rows], x_send.at[half, step, piece],
                      x_recv.at[half, step, piece], next_dev(half))

    unroll = 8
    chip_base = chip * (2 * shard_rows)
    none = jnp.uint32(2 * shard_rows)

    def look_step(step, _):
        for half in (0, 1):
            base = ((chip_at(half, step + 1) * 2 + core) * 2 + half) * half_rows

            def rows_body(i, _):
                at = i * unroll
                for j in range(unroll):
                    row = (ids_ref[base + at + j] - chip_base).astype(jnp.uint32)
                    row = jnp.minimum(row, none).astype(jnp.int32)
                    gath[half, pl.ds(at + j, 1), :] = tab_f32[pl.ds(row, 1), :]
                return 0

            lax.fori_loop(0, half_rows // unroll, rows_body, 0)

        for piece in range(pieces):
            rows = slice(piece * size, (piece + 1) * size)
            for half in (0, 1):
                @pl.when(step == 0)
                def _():
                    xs[half, step, rows] = gath[half, rows].astype(BF16)

                @pl.when(step > 0)
                def _():
                    x_copy(half, step - 1, piece).wait_recv()
                    xs[half, step, rows] = (gath[half, rows] + xs[half, step, rows].astype(F32)).astype(BF16)

                @pl.when(step < steps)
                def _():
                    x_copy(half, step, piece).start()

        @pl.when(step < steps)
        def _():
            gather_step(d_all, d_sems, step)

        @pl.when(step == 0)
        def _():
            setup()

        @pl.when(step > 0)
        def _():
            owned_lists(step)

        return 0

    def setup():
        dw1t_ref[...] = jnp.zeros(dw1t_ref.shape, F32)
        dw2_ref[...] = jnp.zeros(dw2_ref.shape, F32)
        w1_ref[...] = w1t_ref[...].astype(F32).T.astype(BF16)
        w2t_ref[...] = w2_ref[...].astype(F32).T.astype(BF16)
        gain_t[...] = jnp.broadcast_to(gain_ref[...].astype(F32), (dim, dim)).T
        rel = ids_vec[...] - me * shard_rows
        owned = ((rel >= 0) & (rel < shard_rows)).astype(F32).astype(BF16)
        nt = (((1,), (1,)), ((), ()))
        ones = jnp.ones((8, ids_vec.shape[1]), BF16)
        count_ref[...] = lax.dot_general(ones, owned, nt, preferred_element_type=F32).astype(jnp.int32)

    groups = ids_vec.shape[0]
    width = ids_vec.shape[1]
    batch = 8
    turns = groups // batch
    per_step = -(-turns // steps)

    def owned_lists(step):
        lane = lax.broadcasted_iota(jnp.int32, (batch, width), 1)
        sub8 = lax.broadcasted_iota(jnp.int32, (8, width), 0)
        before = (lax.broadcasted_iota(jnp.int32, (width, width), 0)
                  < lax.broadcasted_iota(jnp.int32, (width, width), 1)).astype(F32).astype(BF16)
        place = lax.broadcasted_iota(jnp.int32, (width, width), 0)
        nt = (((1,), (1,)), ((), ()))

        def turn(t, _):
            at = pl.multiple_of(t * batch, batch)
            rel = ids_vec[pl.ds(at, batch), :] - me * shard_rows
            owned = (rel >= 0) & (rel < shard_rows)
            rank = jnp.dot(owned.astype(F32).astype(BF16), before, preferred_element_type=F32).astype(jnp.int32)
            rank = jnp.where(owned, rank, -1)
            rel = jnp.where(owned, rel, 0)
            lines = []
            for g in range(batch):
                hot = (jnp.broadcast_to(rank[g:g + 1], (width, width)) == place).astype(F32).astype(BF16)
                row = jnp.broadcast_to(rel[g:g + 1], (8, width))
                vals = jnp.where(sub8 == 0, lane[:8], jnp.where(sub8 == 1, row // width, row % width))
                got = lax.dot_general(vals.astype(F32).astype(BF16), hot, nt, preferred_element_type=F32)
                got = got.astype(jnp.int32)
                lines.append((got[1:2] * width + got[2:3]) * width + got[0:1])
            list_ref[pl.ds(at, batch), :] = jnp.concatenate(lines, axis=0)
            return 0

        first = jnp.minimum((step - 1) * per_step, turns)
        last = jnp.minimum(step * per_step, turns)
        lax.fori_loop(first, last, turn, 0)

    lax.fori_loop(0, chips, look_step, 0)

    gain = jnp.concatenate([gain_t[...]] * (half_rows // dim), axis=1)
    for half in (0, 1):
        rows_t = xs[half, steps].astype(F32).T
        inv = lax.rsqrt(jnp.mean(rows_t * rows_t, axis=0, keepdims=True) + NORM_EPS)
        x_t[half] = rows_t
        inv_r[half] = inv
        n_all[half, me] = (rows_t * inv * gain).astype(BF16)
        gather_begin(n_all, n_sems, half)

    def d_wait(hop, _):
        for half in (0, 1):
            pair_arrival(d_all, dp_send, dp_recv, half, hop).wait_recv()
        return 0

    lax.fori_loop(0, chips, d_wait, 0)

    nt = (((1,), (1,)), ((), ()))

    def mlp(half, blk, dst):
        def body(i, _):
            cols = pl.ds(pl.multiple_of(i * sub, sub), sub)
            n_t = n_all[half, blk, :, cols]
            d_t = d_all[half, blk, :, cols]
            for lo, hi in tiles:
                u = jnp.dot(w1t_ref[lo:hi], n_t, preferred_element_type=F32).astype(BF16).astype(F32)
                dh = jnp.dot(w2_ref[lo:hi], d_t, preferred_element_type=F32)
                sq = (GELU_C * GELU_A) * (u * u)
                th = jnp.tanh(u * (GELU_C + sq))
                sg = 0.5 + 0.5 * th
                h = u * sg
                slope = sg + (h * (1.0 - th)) * (GELU_C + 3.0 * sq)
                h_buf[lo:hi] = h.astype(BF16)
                du_buf[lo:hi] = (dh * slope).astype(BF16)
            h = h_buf[...]
            du = du_buf[...]
            dst[0, :, cols] = jnp.dot(w2t_ref[...], h, preferred_element_type=F32)
            dst[1, :, cols] = jnp.dot(w1_ref[...], du, preferred_element_type=F32)
            dw2_ref[...] += lax.dot_general(h, d_t, nt, preferred_element_type=F32)
            dw1t_ref[...] += lax.dot_general(du, n_t, nt, preferred_element_type=F32)
            return 0

        lax.fori_loop(0, half_rows // sub, body, 0)

    def p_copy(half, hop):
        return remote(parts.at[(hop % 2) * 2 + half], precv.at[hop, half], p_send.at[hop, half], p_recv.at[hop, half],
                      partner)

    def r_copy(half, val, step):
        return remote(rs.at[step, half, val], rs.at[step + 1, half, val], r_send.at[step, half, val],
                      r_recv.at[step, half, val], next_dev(half))

    def part(g, _):
        early = jnp.where(g < 2, 1, 0)
        turn = jnp.maximum(g - 2, 0)
        step = jnp.where(g < 2, steps, turn // 4)
        late = jnp.where((g >= 2) & (step == steps), 1, 0)
        mine = jnp.where(g < 2, 0, jnp.maximum((turn % 4) // 2, late))
        half = g % 2
        hop = (step + 1) % chips
        blk = chip_at(half, hop) * 2 + (1 - core) * (1 - mine) + core * mine

        ahead = turn // 2
        @pl.when((early == 0) & (half == 0) & (ahead < steps))
        def _():
            gather_step(n_all, n_sems, ahead)

        @pl.when(mine == 0)
        def _():
            pair_arrival(n_all, np_send, np_recv, half, hop).wait_recv()

            @pl.when(hop >= 2)
            def _():
                p_copy(half, hop - 2).wait_send()

        spot = jnp.where(mine == 0, (hop % 2) * 2 + half, 4)
        mlp(half, blk, parts.at[spot])

        @pl.when(mine == 0)
        def _():
            p_copy(half, hop).start()

        @pl.when(mine == 1)
        def _():
            p_copy(half, hop).wait_recv()
            for val in (0, 1):
                @pl.when(step == 0)
                def _():
                    rs[step, half, val] = parts[4, val] + precv[hop, half, val]

                @pl.when(step > 0)
                def _():
                    r_copy(half, val, step - 1).wait_recv()
                    rs[step, half, val] = rs[step, half, val] + (parts[4, val] + precv[hop, half, val])

                @pl.when(step < steps)
                def _():
                    r_copy(half, val, step).start()

        return 0

    lax.fori_loop(0, 4 * chips, part, 0)

    gain = jnp.concatenate([gain_t[...]] * (half_rows // dim), axis=1)
    for half in (0, 1):
        xv = x_t[half]
        inv = inv_r[half]
        rows = slice(half * half_rows, (half + 1) * half_rows)
        scaled = rs[steps, half, 1] * gain
        mean = jnp.mean(xv * scaled, axis=0, keepdims=True)
        dx = inv * (scaled - xv * inv * inv * mean)
        dx = dout_ref[rows, :].astype(F32) + dx.T
        dx_all[half, me] = dx.astype(BF16)
        gather_begin(dx_all, e_sems, half)
    for half in (0, 1):
        rows = slice(half * half_rows, (half + 1) * half_rows)
        out_ref[rows, :] = (x_t[half] + rs[steps, half, 0]).T.astype(BF16)

    def e_step(step, _):
        gather_step(dx_all, e_sems, step)
        return 0

    lax.fori_loop(0, steps, e_step, 0)

    for buf, sems in ((d_all, d_sems), (n_all, n_sems)):
        gather_drain(buf, sems)

    def drain(step, _):
        for half in (0, 1):
            for piece in range(pieces):
                x_copy(half, step, piece).wait_send()
            for val in (0, 1):
                r_copy(half, val, step).wait_send()
        return 0

    lax.fori_loop(0, steps, drain, 0)
    for half in (0, 1):
        for hop in (chips - 2, chips - 1):
            p_copy(half, hop).wait_send()
    gather_drain(dx_all, e_sems)

    def e_wait(hop, _):
        for half in (0, 1):
            pair_arrival(dx_all, ep_send, ep_recv, half, hop).wait_recv()
        return 0

    lax.fori_loop(0, chips, e_wait, 0)


def row_tiles(hidden):
    if hidden < 256:
        return ((0, hidden),)
    cut = (hidden // 2) // 16 * 16
    return ((0, cut), (cut, hidden))


def run_block(chips, ids, table, gain, w_up, w_down, d_out):
    rows, dim = d_out.shape
    shard_rows = table.shape[0]
    hidden = w_down.shape[0]
    half = rows // 2
    devs = 2 * chips
    sub = min(256, half)
    dma = pltpu.SemaphoreType.DMA
    vmem = pl.BlockSpec(memory_space=pltpu.VMEM)
    tokens = rows * devs
    groups = tokens // dim

    def gather_sems(pieces):
        ring, pair = (2, chips - 1, pieces), (2, chips)
        return [dma(ring), dma(ring), dma(pair), dma(pair)]

    return pl.pallas_call(
        functools.partial(block_kernel, chips, sub, row_tiles(hidden)),
        out_shape=(
            jax.ShapeDtypeStruct((rows, dim), BF16),
            jax.ShapeDtypeStruct((hidden, dim), F32),
            jax.ShapeDtypeStruct((hidden, dim), F32),
            jax.ShapeDtypeStruct((2, devs, half, dim), BF16),
            jax.ShapeDtypeStruct((groups, dim), jnp.int32),
            jax.ShapeDtypeStruct((8, groups), jnp.int32),
        ),
        in_specs=[pl.BlockSpec(memory_space=pltpu.SMEM)] + [vmem] * 6,
        out_specs=(vmem,) * 6,
        scratch_shapes=[
            pltpu.VMEM((shard_rows, dim), BF16),
            pltpu.VMEM((2 * shard_rows + 8, dim), F32),
            pltpu.VMEM((2, half, dim), F32),
            pltpu.VMEM((2, chips, half, dim), BF16),
            pltpu.VMEM((2, dim, half), F32),
            pltpu.VMEM((2, 1, half), F32),
            pltpu.VMEM((dim, dim), F32),
            pltpu.VMEM((dim, hidden), BF16),
            pltpu.VMEM((dim, hidden), BF16),
            pltpu.VMEM((2, devs, dim, half), BF16),
            pltpu.VMEM((2, devs, dim, half), BF16),
            pltpu.VMEM((hidden, sub), BF16),
            pltpu.VMEM((hidden, sub), BF16),
            pltpu.VMEM((5, 2, dim, half), F32),
            pltpu.VMEM((chips, 2, 2, dim, half), F32),
            pltpu.VMEM((chips, 2, 2, dim, half), F32),
            dma((2,)),
            dma((2, chips - 1, 2)), dma((2, chips - 1, 2)),
            *gather_sems(1), *gather_sems(2), *gather_sems(4),
            dma((chips, 2)), dma((chips, 2)),
            dma((chips - 1, 2, 2)), dma((chips - 1, 2, 2)),
        ],
        compiler_params=pltpu.CompilerParams(
            collective_id=0, has_side_effects=True, vmem_limit_bytes=67043328,
        ),
        cost_estimate=pl.CostEstimate(flops=12 * tokens * hidden * dim, bytes_accessed=tokens * dim * 8,
                                      transcendentals=0),
        name="block",
    )(ids, ids.reshape(groups, dim), table, gain.reshape(1, dim), w_up.T, w_down, d_out)


def scatter_kernel(
    half_rows, extra,
    list_ref, count_ref, dx_ref, *refs,
):
    extra_in, grad_ref, extra_out = refs[:extra], refs[extra], refs[extra + 1:2 * extra + 1]
    acc, dx_in, dx_f32, in_sem, ex_sem = refs[2 * extra + 1:2 * extra + 6]
    extra_buf = refs[2 * extra + 6:]
    blocks, block = dx_in.shape[:2]
    groups, width = list_ref.shape
    tokens = dx_f32.shape[0]

    def load(b):
        return pltpu.make_async_copy(dx_ref.at[pl.ds(b * block, block)], dx_in.at[b], in_sem.at[b])

    def take(e):
        return pltpu.make_async_copy(extra_in[e], extra_buf[e], ex_sem.at[0, e])

    def give(e):
        return pltpu.make_async_copy(extra_buf[e], extra_out[e], ex_sem.at[1, e])

    for b in range(blocks):
        load(b).start()
    for e in range(extra):
        take(e).start()
    acc[...] = jnp.zeros(acc.shape, F32)
    conv = 128

    for b in range(blocks):
        load(b).wait()

        def convert(i, _):
            at = pl.multiple_of(i * conv, conv)
            dst = pl.multiple_of(b * block + i * conv, conv)
            dx_f32[pl.ds(dst, conv), :] = dx_in[b, pl.ds(at, conv), :].astype(F32)
            return 0

        lax.fori_loop(0, block // conv, convert, 0)
    for e in range(extra):
        take(e).wait()
        give(e).start()

    def group(g, _):
        start = g * width
        first = ((start // half_rows) % 2) * (tokens // 2) + (start // (2 * half_rows)) * half_rows + start % half_rows

        def one(i, _):
            packed = list_ref[g, i]
            tok = first + (packed & (width - 1))
            row = packed >> (width.bit_length() - 1)
            acc[pl.ds(row, 1), :] += dx_f32[pl.ds(tok, 1), :]
            return 0

        lax.fori_loop(0, count_ref[0, g], one, 0)
        return 0

    lax.fori_loop(0, groups, group, 0)
    copy = pltpu.make_async_copy(acc, grad_ref, in_sem.at[0])
    copy.start()
    for e in range(extra):
        give(e).wait()
    copy.wait()


def scatter_rows(half_rows, shard_rows, lists, counts, dx_all, others):
    tokens, dim = dx_all.shape
    smem = pl.BlockSpec(memory_space=pltpu.SMEM)
    hbm = pl.BlockSpec(memory_space=pltpu.HBM)
    blocks = 8
    extra = len(others)
    shapes = [jax.ShapeDtypeStruct((shard_rows, dim), F32)] + [jax.ShapeDtypeStruct(o.shape, o.dtype) for o in others]
    return pl.pallas_call(
        functools.partial(scatter_kernel, half_rows, extra),
        out_shape=tuple(shapes),
        in_specs=[smem, smem] + [hbm] * (1 + extra),
        out_specs=(hbm,) * (1 + extra),
        scratch_shapes=[
            pltpu.VMEM((shard_rows, dim), F32),
            pltpu.VMEM((blocks, tokens // blocks, dim), BF16),
            pltpu.VMEM((tokens, dim), F32),
            pltpu.SemaphoreType.DMA((blocks,)),
            pltpu.SemaphoreType.DMA((2, extra)),
            *[pltpu.VMEM(o.shape, o.dtype) for o in others],
        ],
        compiler_params=pltpu.CompilerParams(vmem_limit_bytes=67043328),
        name="scatter",
    )(lists, counts, dx_all, *others)


def solution(mesh):
    chips = mesh.shape["tp"] // 2

    def shard_body(token_ids, embed_table, norm_gain, w_up, w_down, d_out):
        shard_rows, dim = embed_table.shape
        block_out, dw1t, dw2, dx_all, lists, counts = run_block(
            chips, token_ids, embed_table, norm_gain, w_up, w_down, d_out)
        grad_table, block_out, dw1t, dw2 = scatter_rows(
            d_out.shape[0] // 2, shard_rows, lists, counts, dx_all.reshape(-1, dim), (block_out, dw1t, dw2))
        return block_out, grad_table, dw1t.T, dw2

    return jax.shard_map(
        shard_body,
        mesh=mesh,
        in_specs=(P("dp"), P("tp", None), P(), P(None, "tp"), P("tp", None), P(("dp", "tp"), None)),
        out_specs=(P(("dp", "tp"), None), P(("dp", "tp"), None), P("dp", "tp"), P(("dp", "tp"), None)),
        check_vma=False,
    )
```

```python
import functools

import jax
import jax.numpy as jnp
from jax import lax
from jax.experimental import pallas as pl
from jax.experimental.pallas import tpu as pltpu
from jax.sharding import PartitionSpec as P

NORM_EPS = 1e-6
GELU_C = 0.7978845608028654
GELU_A = 0.044715
BUNCH = 4
MESH = pl.DeviceIdType.MESH
F32 = jnp.float32
BF16 = jnp.bfloat16


def remote(src, dst, send_sem, recv_sem, dev):
    return pltpu.make_async_remote_copy(
        src_ref=src, dst_ref=dst, send_sem=send_sem, recv_sem=recv_sem,
        device_id={"tp": dev}, device_id_type=MESH,
    )


def block_kernel(
    chips, tiles,
    ids_ref, ids_vec, table_hbm, gain_ref, w1t_ref, w2_ref, dout_ref,
    out_hbm, dw1t_hbm, dw2_hbm, dx_hbm, list_hbm, count_hbm,
    out_ref, dw1t_ref, dw2_ref, dx_all, list_ref, count_ref,
    table_ref, tab_in, tab_f32, gath, xs, x_t, inv_r, gain_t, w1_ref, w2t_ref, d_all, n_all,
    h_a, h_b, du_a, du_b, parts, precv, rs,
    tab_sem, put_sem, dx_sem, x_send, x_recv, d_send, d_recv, dp_send, dp_recv, n_send, n_recv, np_send, np_recv,
    e_send, e_recv, ep_send, ep_recv, p_send, p_recv, r_send, r_recv,
):
    me = lax.axis_index("tp")
    chip, core = me // 2, me % 2
    partner = chip * 2 + 1 - core
    up = ((chip + 1) % chips) * 2 + core
    down = ((chip + chips - 1) % chips) * 2 + core
    half_rows, dim = gath.shape[1:]
    shard_rows = table_ref.shape[0]
    steps = chips - 1

    def next_dev(half):
        return up * (1 - half) + down * half

    def chip_at(half, hop):
        return (chip + (1 - half) * (chips - hop) + half * hop) % chips

    tab_load = pltpu.make_async_copy(table_hbm, table_ref, tab_sem.at[2])
    tab_load.start()
    barrier = pltpu.get_barrier_semaphore()
    for dev in (partner, up, down):
        pl.semaphore_signal(barrier, inc=1, device_id={"tp": dev}, device_id_type=MESH)
    pl.semaphore_wait(barrier, 3)

    def ring_copy(buf, send, recv, half, hop, step, piece):
        blk = chip_at(half, hop) * 2 + core
        pieces = send.shape[2]
        size = buf.shape[2] // pieces
        ref = buf.at[half, blk, pl.ds(piece * size, size)]
        return remote(ref, ref, send.at[half, step, piece], recv.at[half, step, piece], next_dev(half))

    def pair_copy(buf, send, recv, half, hop):
        blk = chip_at(half, hop) * 2 + core
        return remote(buf.at[half, blk], buf.at[half, blk], send.at[half, hop], recv.at[half, hop], partner)

    def pair_arrival(buf, send, recv, half, hop):
        blk = chip_at(half, hop) * 2 + 1 - core
        return remote(buf.at[half, blk], buf.at[half, blk], send.at[half, hop], recv.at[half, hop], partner)

    def gather_begin(buf, sems, half):
        send, recv, psend_, precv_ = sems
        for piece in range(send.shape[2]):
            ring_copy(buf, send, recv, half, 0, 0, piece).start()
        pair_copy(buf, psend_, precv_, half, 0).start()

    def gather_step(buf, sems, step):
        send, recv, psend_, precv_ = sems
        for piece in range(send.shape[2]):
            for half in (0, 1):
                ring_copy(buf, send, recv, half, step + 1, step, piece).wait_recv()

                @pl.when(step + 1 < steps)
                def _():
                    ring_copy(buf, send, recv, half, step + 1, step + 1, piece).start()

        for half in (0, 1):
            pair_copy(buf, psend_, precv_, half, step + 1).start()

    def gather_drain(buf, sems):
        send, recv, psend_, precv_ = sems

        def body(step, _):
            for half in (0, 1):
                for piece in range(send.shape[2]):
                    ring_copy(buf, send, recv, half, step, step, piece).wait_send()
            return 0

        lax.fori_loop(0, steps, body, 0)

        def pair_body(hop, _):
            for half in (0, 1):
                pair_copy(buf, psend_, precv_, half, hop).wait_send()
            return 0

        lax.fori_loop(0, chips, pair_body, 0)

    d_sems = (d_send, d_recv, dp_send, dp_recv)
    n_sems = (n_send, n_recv, np_send, np_recv)
    e_sems = (e_send, e_recv, ep_send, ep_recv)

    tab_copy = remote(table_hbm, tab_in, tab_sem.at[0], tab_sem.at[1], partner)
    tab_copy.start()
    for half in (0, 1):
        rows = dout_ref[half * half_rows:(half + 1) * half_rows, :].astype(F32)
        d_all[half, me] = rows.T.astype(BF16)
        gather_begin(d_all, d_sems, half)
    conv = 32

    def convert(src, start):
        def body(i, _):
            at = pl.multiple_of(i * conv, conv)
            dst = pl.multiple_of(start + i * conv, conv)
            tab_f32[pl.ds(dst, conv), :] = src[pl.ds(at, conv), :].astype(F32)
            return 0

        lax.fori_loop(0, shard_rows // conv, body, 0)

    tab_load.wait()
    convert(table_ref, core * shard_rows)
    tab_f32[pl.ds(2 * shard_rows, 8), :] = jnp.zeros((8, dim), F32)
    gather_step(d_all, d_sems, 0)
    tab_copy.wait()
    convert(tab_in, (1 - core) * shard_rows)
    gather_step(d_all, d_sems, 1)

    pieces = x_send.shape[2]
    size = half_rows // pieces

    def x_copy(half, step, piece):
        rows = pl.ds(piece * size, size)
        return remote(xs.at[half, step, rows], xs.at[half, step + 1, rows], x_send.at[half, step, piece],
                      x_recv.at[half, step, piece], next_dev(half))

    unroll = 8
    chip_base = chip * (2 * shard_rows)
    none = jnp.uint32(2 * shard_rows)

    def look_step(step, _):
        for half in (0, 1):
            base = ((chip_at(half, step + 1) * 2 + core) * 2 + half) * half_rows

            def rows_body(i, _):
                at = i * unroll
                for j in range(unroll):
                    row = (ids_ref[base + at + j] - chip_base).astype(jnp.uint32)
                    row = jnp.minimum(row, none).astype(jnp.int32)
                    gath[half, pl.ds(at + j, 1), :] = tab_f32[pl.ds(row, 1), :]
                return 0

            lax.fori_loop(0, half_rows // unroll, rows_body, 0)

        for piece in range(pieces):
            rows = slice(piece * size, (piece + 1) * size)
            for half in (0, 1):
                @pl.when(step == 0)
                def _():
                    xs[half, step, rows] = gath[half, rows].astype(BF16)

                @pl.when(step > 0)
                def _():
                    x_copy(half, step - 1, piece).wait_recv()
                    xs[half, step, rows] = (gath[half, rows] + xs[half, step, rows].astype(F32)).astype(BF16)

                @pl.when(step < steps)
                def _():
                    x_copy(half, step, piece).start()

        @pl.when(step + 2 < steps)
        def _():
            gather_step(d_all, d_sems, step + 2)

        @pl.when(step == 0)
        def _():
            setup()

        @pl.when(step > 0)
        def _():
            owned_lists(step)

        return 0

    def setup():
        dw1t_ref[...] = jnp.zeros(dw1t_ref.shape, F32)
        dw2_ref[...] = jnp.zeros(dw2_ref.shape, F32)
        w1_ref[...] = w1t_ref[...].astype(F32).T.astype(BF16)
        w2t_ref[...] = w2_ref[...].astype(F32).T.astype(BF16)
        gain_t[...] = jnp.broadcast_to(gain_ref[...].astype(F32), (dim, dim)).T
        rel = ids_vec[...] - me * shard_rows
        owned = ((rel >= 0) & (rel < shard_rows)).astype(F32).astype(BF16)
        nt = (((1,), (1,)), ((), ()))
        ones = jnp.ones((8, ids_vec.shape[1]), BF16)
        counts = lax.dot_general(ones, owned, nt, preferred_element_type=F32).astype(jnp.int32)
        count_ref[...] = (counts + (BUNCH - 1)) // BUNCH

    groups = ids_vec.shape[0]
    width = ids_vec.shape[1]
    tokens = groups * width
    batch = 8
    turns = groups // batch
    per_step = -(-turns // steps)

    def owned_lists(step):
        lane = lax.broadcasted_iota(jnp.int32, (batch, width), 1)
        sub8 = lax.broadcasted_iota(jnp.int32, (8, width), 0)
        before = (lax.broadcasted_iota(jnp.int32, (width, width), 0)
                  < lax.broadcasted_iota(jnp.int32, (width, width), 1)).astype(F32).astype(BF16)
        place = lax.broadcasted_iota(jnp.int32, (width, width), 0)
        nt = (((1,), (1,)), ((), ()))

        def turn(t, _):
            at = pl.multiple_of(t * batch, batch)
            rel = ids_vec[pl.ds(at, batch), :] - me * shard_rows
            owned = (rel >= 0) & (rel < shard_rows)
            rank = jnp.dot(owned.astype(F32).astype(BF16), before, preferred_element_type=F32).astype(jnp.int32)
            rank = jnp.where(owned, rank, -1)
            rel = jnp.where(owned, rel, 0)
            count = jnp.sum(owned.astype(F32), axis=1, keepdims=True).astype(jnp.int32)
            lines = []
            for g in range(batch):
                hot = (jnp.broadcast_to(rank[g:g + 1], (width, width)) == place).astype(F32).astype(BF16)
                row = jnp.broadcast_to(rel[g:g + 1], (8, width))
                vals = jnp.where(sub8 == 0, lane[:8], jnp.where(sub8 == 1, row // width, row % width))
                got = lax.dot_general(vals.astype(F32).astype(BF16), hot, nt, preferred_element_type=F32)
                got = got.astype(jnp.int32)
                start = (t * batch + g) * width
                place_0 = (((start // half_rows) % 2) * (tokens // 2) + (start // (2 * half_rows)) * half_rows
                           + start % half_rows)
                line = (got[1:2] * width + got[2:3]) * tokens + (got[0:1] + place_0)
                lines.append(jnp.where(lane[:1] < count[g:g + 1], line, shard_rows * tokens))
            list_ref[pl.ds(at, batch), :] = jnp.concatenate(lines, axis=0)
            return 0

        first = jnp.minimum((step - 1) * per_step, turns)
        last = jnp.minimum(step * per_step, turns)
        lax.fori_loop(first, last, turn, 0)

    lax.fori_loop(0, chips, look_step, 0)

    gain = jnp.concatenate([gain_t[...]] * (half_rows // dim), axis=1)
    for half in (0, 1):
        rows_t = xs[half, steps].astype(F32).T
        inv = lax.rsqrt(jnp.mean(rows_t * rows_t, axis=0, keepdims=True) + NORM_EPS)
        x_t[half] = rows_t
        inv_r[half] = inv
        n_all[half, me] = (rows_t * inv * gain).astype(BF16)
        gather_begin(n_all, n_sems, half)

    def d_wait(hop, _):
        for half in (0, 1):
            pair_arrival(d_all, dp_send, dp_recv, half, hop).wait_recv()
        return 0

    lax.fori_loop(0, chips, d_wait, 0)

    nt = (((1,), (1,)), ((), ()))

    def mlp(half, blk, dst):
        sub = half_rows // 2
        left, right = slice(0, sub), slice(sub, 2 * sub)

        def front(lo, hi, cols, h_buf, du_buf):
            u = jnp.dot(w1t_ref[lo:hi], n_all[half, blk, :, cols], preferred_element_type=F32).astype(BF16).astype(F32)
            dh = jnp.dot(w2_ref[lo:hi], d_all[half, blk, :, cols], preferred_element_type=F32)
            sq = (GELU_C * GELU_A) * (u * u)
            th = jnp.tanh(u * (GELU_C + sq))
            sg = 0.5 + 0.5 * th
            h = u * sg
            slope = sg + (h * (1.0 - th)) * (GELU_C + 3.0 * sq)
            h_buf[lo:hi] = h.astype(BF16)
            du_buf[lo:hi] = (dh * slope).astype(BF16)

        def weights(lo, hi, cols, h_buf, du_buf):
            n_t, d_t = n_all[half, blk, :, cols], d_all[half, blk, :, cols]
            dw2_ref[lo:hi] += lax.dot_general(h_buf[lo:hi], d_t, nt, preferred_element_type=F32)
            dw1t_ref[lo:hi] += lax.dot_general(du_buf[lo:hi], n_t, nt, preferred_element_type=F32)

        def back(cols, h_buf, du_buf):
            dst[0, :, cols] = jnp.dot(w2t_ref[...], h_buf[...], preferred_element_type=F32)
            dst[1, :, cols] = jnp.dot(w1_ref[...], du_buf[...], preferred_element_type=F32)

        for lo, hi in tiles:
            front(lo, hi, left, h_a, du_a)
        for lo, hi in tiles:
            weights(lo, hi, left, h_a, du_a)
            front(lo, hi, right, h_b, du_b)
        back(left, h_a, du_a)
        for lo, hi in tiles:
            weights(lo, hi, right, h_b, du_b)
        back(right, h_b, du_b)

    def order_of(half, hop):
        return (hop + half * (chips - 1)) % chips

    def p_copy(half, hop):
        return remote(parts.at[(order_of(half, hop) % 2) * 2 + half], precv.at[hop, half], p_send.at[hop, half],
                      p_recv.at[hop, half], partner)

    def r_copy(half, val, step):
        return remote(rs.at[step, half, val], rs.at[step + 1, half, val], r_send.at[step, half, val],
                      r_recv.at[step, half, val], next_dev(half))

    def part(g, _):
        turn = jnp.maximum(g - 1, 0)
        own_chip = jnp.where((g == 0) | (turn >= 4 * steps), 1, 0)
        late = turn - 4 * steps
        step = jnp.where(own_chip == 1, steps, turn // 4)
        half = jnp.where(own_chip == 1, jnp.where((late == 0) | (late == 2), 1, 0), (turn % 4) // 2)
        mine = jnp.where(own_chip == 1, jnp.where(late >= 1, 1, 0), turn % 2)
        hop = (step + 1) % chips
        blk = chip_at(half, hop) * 2 + (1 - core) * (1 - mine) + core * mine

        lead = min(3, steps)
        early = (g == 1) | ((g == 2) & (lead > 1)) | ((g == 4) & (lead > 2))
        steady = (turn % 4 == 0) & (turn >= 8) & (turn // 4 + 1 < steps)
        ahead = jnp.where(early, jnp.where(g == 4, 2, g - 1), turn // 4 + 1)

        @pl.when(early | steady)
        def _():
            gather_step(n_all, n_sems, ahead)

        @pl.when(mine == 0)
        def _():
            pair_arrival(n_all, np_send, np_recv, half, hop).wait_recv()

            @pl.when(order_of(half, hop) >= 2)
            def _():
                p_copy(half, (hop + chips - 2) % chips).wait_send()

        spot = jnp.where(mine == 0, (order_of(half, hop) % 2) * 2 + half, 4)
        mlp(half, blk, parts.at[spot])

        @pl.when(mine == 0)
        def _():
            p_copy(half, hop).start()

        @pl.when(mine == 1)
        def _():
            p_copy(half, hop).wait_recv()
            for val in (0, 1):
                @pl.when(step == 0)
                def _():
                    rs[step, half, val] = parts[4, val] + precv[hop, half, val]

                @pl.when(step > 0)
                def _():
                    r_copy(half, val, step - 1).wait_recv()
                    rs[step, half, val] = rs[step, half, val] + (parts[4, val] + precv[hop, half, val])

                @pl.when(step < steps)
                def _():
                    r_copy(half, val, step).start()

        return 0

    lax.fori_loop(0, 4 * chips, part, 0)

    puts = [
        pltpu.make_async_copy(src, dst, put_sem.at[i])
        for i, (src, dst) in enumerate((
            (dw1t_ref, dw1t_hbm), (dw2_ref, dw2_hbm), (list_ref, list_hbm), (count_ref, count_hbm), (out_ref, out_hbm),
        ))
    ]
    for put in puts[:4]:
        put.start()

    def dx_put(half, blk):
        return pltpu.make_async_copy(dx_all.at[half, blk], dx_hbm.at[half, blk], dx_sem.at[half, blk])

    gain = jnp.concatenate([gain_t[...]] * (half_rows // dim), axis=1)
    for half in (0, 1):
        xv = x_t[half]
        inv = inv_r[half]
        rows = slice(half * half_rows, (half + 1) * half_rows)
        scaled = rs[steps, half, 1] * gain
        mean = jnp.mean(xv * scaled, axis=0, keepdims=True)
        dx = inv * (scaled - xv * inv * inv * mean)
        dx = dout_ref[rows, :].astype(F32) + dx.T
        dx_all[half, me] = dx.astype(BF16)
        gather_begin(dx_all, e_sems, half)
        dx_put(half, me).start()
    for half in (0, 1):
        rows = slice(half * half_rows, (half + 1) * half_rows)
        out_ref[rows, :] = (x_t[half] + rs[steps, half, 0]).T.astype(BF16)

    puts[4].start()

    def pair_done(hop):
        for half in (0, 1):
            pair_arrival(dx_all, ep_send, ep_recv, half, hop).wait_recv()
            dx_put(half, chip_at(half, hop) * 2 + 1 - core).start()

    def e_step(step, _):
        gather_step(dx_all, e_sems, step)
        for half in (0, 1):
            dx_put(half, chip_at(half, step + 1) * 2 + core).start()
        pair_done(step)
        return 0

    lax.fori_loop(0, steps, e_step, 0)

    for buf, sems in ((d_all, d_sems), (n_all, n_sems)):
        gather_drain(buf, sems)

    def drain(step, _):
        for half in (0, 1):
            for piece in range(pieces):
                x_copy(half, step, piece).wait_send()
            for val in (0, 1):
                r_copy(half, val, step).wait_send()
        return 0

    lax.fori_loop(0, steps, drain, 0)
    for half in (0, 1):
        for order in (chips - 2, chips - 1):
            p_copy(half, (order + half) % chips).wait_send()
    for put in puts:
        put.wait()
    pair_done(steps)
    gather_drain(dx_all, e_sems)

    def put_wait(blk, _):
        for half in (0, 1):
            dx_put(half, blk).wait()
        return 0

    lax.fori_loop(0, 2 * chips, put_wait, 0)


def row_tiles(hidden):
    count = 4 if hidden >= 512 else 1
    cut = -(-hidden // (16 * count)) * 16
    edges = [min(i * cut, hidden) for i in range(count)] + [hidden]
    return tuple(zip(edges[:-1], edges[1:]))


def run_block(chips, ids, table, gain, w_up, w_down, d_out):
    rows, dim = d_out.shape
    shard_rows = table.shape[0]
    hidden = w_down.shape[0]
    half = rows // 2
    devs = 2 * chips
    sub = half // 2
    dma = pltpu.SemaphoreType.DMA
    vmem = pl.BlockSpec(memory_space=pltpu.VMEM)
    tokens = rows * devs
    groups = tokens // dim

    def gather_sems(pieces):
        ring, pair = (2, chips - 1, pieces), (2, chips)
        return [dma(ring), dma(ring), dma(pair), dma(pair)]

    results = (
        jax.ShapeDtypeStruct((rows, dim), BF16),
        jax.ShapeDtypeStruct((hidden, dim), F32),
        jax.ShapeDtypeStruct((hidden, dim), F32),
        jax.ShapeDtypeStruct((2, devs, half, dim), BF16),
        jax.ShapeDtypeStruct((groups, dim), jnp.int32),
        jax.ShapeDtypeStruct((8, groups), jnp.int32),
    )
    hbm = pl.BlockSpec(memory_space=pltpu.HBM)
    return pl.pallas_call(
        functools.partial(block_kernel, chips, row_tiles(hidden)),
        out_shape=results,
        in_specs=[pl.BlockSpec(memory_space=pltpu.SMEM), vmem, hbm] + [vmem] * 4,
        out_specs=(hbm,) * 6,
        scratch_shapes=[
            *[pltpu.VMEM(r.shape, r.dtype) for r in results],
            pltpu.VMEM((shard_rows, dim), BF16),
            pltpu.VMEM((shard_rows, dim), BF16),
            pltpu.VMEM((2 * shard_rows + 8, dim), F32),
            pltpu.VMEM((2, half, dim), F32),
            pltpu.VMEM((2, chips, half, dim), BF16),
            pltpu.VMEM((2, dim, half), F32),
            pltpu.VMEM((2, 1, half), F32),
            pltpu.VMEM((dim, dim), F32),
            pltpu.VMEM((dim, hidden), BF16),
            pltpu.VMEM((dim, hidden), BF16),
            pltpu.VMEM((2, devs, dim, half), BF16),
            pltpu.VMEM((2, devs, dim, half), BF16),
            *[pltpu.VMEM((hidden, sub), BF16)] * 4,
            pltpu.VMEM((5, 2, dim, half), F32),
            pltpu.VMEM((chips, 2, 2, dim, half), F32),
            pltpu.VMEM((chips, 2, 2, dim, half), F32),
            dma((3,)), dma((5,)), dma((2, devs)),
            dma((2, chips - 1, 2)), dma((2, chips - 1, 2)),
            *gather_sems(1), *gather_sems(2), *gather_sems(4),
            dma((chips, 2)), dma((chips, 2)),
            dma((chips - 1, 2, 2)), dma((chips - 1, 2, 2)),
        ],
        compiler_params=pltpu.CompilerParams(
            collective_id=0, has_side_effects=True, vmem_limit_bytes=67043328,
        ),
        cost_estimate=pl.CostEstimate(flops=12 * tokens * hidden * dim, bytes_accessed=tokens * dim * 8,
                                      transcendentals=0),
        name="block",
    )(ids, ids.reshape(groups, dim), table, gain.reshape(1, dim), w_up.T, w_down, d_out)


def scatter_kernel(extra, list_hbm, count_hbm, dx_ref, *refs):
    extra_in, grad_ref, extra_out = refs[:extra], refs[extra], refs[extra + 1:2 * extra + 1]
    acc, dx_in, dx_f32, list_ref, count_ref, in_sem, ex_sem, small_sem = refs[2 * extra + 1:2 * extra + 9]
    extra_buf = refs[2 * extra + 9:]
    blocks, block = dx_in.shape[:2]
    groups = list_ref.shape[0]
    tokens = dx_f32.shape[0]
    shard_rows = grad_ref.shape[0]
    shift = tokens.bit_length() - 1

    def load(b):
        return pltpu.make_async_copy(dx_ref.at[pl.ds(b * block, block)], dx_in.at[b], in_sem.at[b])

    def take(e):
        return pltpu.make_async_copy(extra_in[e], extra_buf[e], ex_sem.at[0, e])

    def give(e):
        return pltpu.make_async_copy(extra_buf[e], extra_out[e], ex_sem.at[1, e])

    small = (
        pltpu.make_async_copy(list_hbm, list_ref, small_sem.at[0]),
        pltpu.make_async_copy(count_hbm, count_ref, small_sem.at[1]),
    )
    for copy in small:
        copy.start()
    for b in range(blocks):
        load(b).start()
    for e in range(extra):
        take(e).start()
    acc[...] = jnp.zeros(acc.shape, F32)
    conv = 128

    for b in range(blocks):
        load(b).wait()

        def convert(i, _):
            at = pl.multiple_of(i * conv, conv)
            dst = pl.multiple_of(b * block + i * conv, conv)
            dx_f32[pl.ds(dst, conv), :] = dx_in[b, pl.ds(at, conv), :].astype(F32)
            return 0

        lax.fori_loop(0, block // conv, convert, 0)
    for e in range(extra):
        take(e).wait()
        give(e).start()
    for copy in small:
        copy.wait()

    def group(g, _):
        def bunch(i, _):
            for j in range(BUNCH):
                packed = list_ref[g, i * BUNCH + j]
                acc[pl.ds(packed >> shift, 1), :] += dx_f32[pl.ds(packed & (tokens - 1), 1), :]
            return 0

        lax.fori_loop(0, count_ref[0, g], bunch, 0)
        return 0

    lax.fori_loop(0, groups, group, 0)
    copy = pltpu.make_async_copy(acc.at[pl.ds(0, shard_rows)], grad_ref, in_sem.at[0])
    copy.start()
    for e in range(extra):
        give(e).wait()
    copy.wait()


def scatter_rows(shard_rows, lists, counts, dx_all, others):
    tokens, dim = dx_all.shape
    hbm = pl.BlockSpec(memory_space=pltpu.HBM)
    blocks = 8
    extra = len(others)
    shapes = [jax.ShapeDtypeStruct((shard_rows, dim), F32)] + [jax.ShapeDtypeStruct(o.shape, o.dtype) for o in others]
    return pl.pallas_call(
        functools.partial(scatter_kernel, extra),
        out_shape=tuple(shapes),
        in_specs=[hbm] * (3 + extra),
        out_specs=(hbm,) * (1 + extra),
        scratch_shapes=[
            pltpu.VMEM((shard_rows + 8, dim), F32),
            pltpu.VMEM((blocks, tokens // blocks, dim), BF16),
            pltpu.VMEM((tokens, dim), F32),
            pltpu.SMEM(lists.shape, jnp.int32),
            pltpu.SMEM(counts.shape, jnp.int32),
            pltpu.SemaphoreType.DMA((blocks,)),
            pltpu.SemaphoreType.DMA((2, extra)),
            pltpu.SemaphoreType.DMA((2,)),
            *[pltpu.VMEM(o.shape, o.dtype) for o in others],
        ],
        compiler_params=pltpu.CompilerParams(vmem_limit_bytes=67043328),
        name="scatter",
    )(lists, counts, dx_all, *others)


def solution(mesh):
    chips = mesh.shape["tp"] // 2

    def shard_body(token_ids, embed_table, norm_gain, w_up, w_down, d_out):
        shard_rows, dim = embed_table.shape
        block_out, dw1t, dw2, dx_all, lists, counts = run_block(
            chips, token_ids, embed_table, norm_gain, w_up, w_down, d_out)
        grad_table, block_out, dw1t, dw2 = scatter_rows(
            shard_rows, lists, counts, dx_all.reshape(-1, dim), (block_out, dw1t, dw2))
        return block_out, grad_table, dw1t.T, dw2

    return jax.shard_map(
        shard_body,
        mesh=mesh,
        in_specs=(P("dp"), P("tp", None), P(), P(None, "tp"), P("tp", None), P(("dp", "tp"), None)),
        out_specs=(P(("dp", "tp"), None), P(("dp", "tp"), None), P("dp", "tp"), P(("dp", "tp"), None)),
        check_vma=False,
    )
```

```python
import functools

import jax
import jax.numpy as jnp
from jax import lax
from jax.experimental import pallas as pl
from jax.experimental.pallas import tpu as pltpu
from jax.sharding import PartitionSpec as P

NORM_EPS = 1e-6
GELU_C = 0.7978845608028654
GELU_A = 0.044715
BUNCH = 4
MESH = pl.DeviceIdType.MESH
F32 = jnp.float32
BF16 = jnp.bfloat16


def remote(src, dst, send_sem, recv_sem, dev):
    return pltpu.make_async_remote_copy(
        src_ref=src, dst_ref=dst, send_sem=send_sem, recv_sem=recv_sem,
        device_id={"tp": dev}, device_id_type=MESH,
    )


def block_kernel(
    chips, tiles,
    ids_ref, ids_vec, table_hbm, gain_ref, w1t_ref, w2_ref, dout_ref,
    out_hbm, dw1t_hbm, dw2_hbm, dx_hbm, list_hbm, count_hbm,
    out_ref, dw1t_ref, dw2_ref, dx_all, list_ref, count_ref,
    table_ref, tab_in, tab_f32, gath, xs, x_t, inv_r, gain_t, w1_ref, w2t_ref, d_all, n_all,
    h_a, h_b, du_a, du_b, parts, precv, rs,
    tab_sem, put_sem, dx_sem, x_send, x_recv, d_send, d_recv, dp_send, dp_recv, n_send, n_recv, np_send, np_recv,
    e_send, e_recv, ep_send, ep_recv, p_send, p_recv, r_send, r_recv,
):
    me = lax.axis_index("tp")
    chip, core = me // 2, me % 2
    partner = chip * 2 + 1 - core
    up = ((chip + 1) % chips) * 2 + core
    down = ((chip + chips - 1) % chips) * 2 + core
    half_rows, dim = gath.shape[1:]
    shard_rows = table_ref.shape[0]
    steps = chips - 1

    def next_dev(half):
        return up * (1 - half) + down * half

    def chip_at(half, hop):
        return (chip + (1 - half) * (chips - hop) + half * hop) % chips

    tab_load = pltpu.make_async_copy(table_hbm, table_ref, tab_sem.at[2])
    tab_load.start()
    with jax.named_scope("s_entry"):
        barrier = pltpu.get_barrier_semaphore()
        for dev in (partner, up, down):
            pl.semaphore_signal(barrier, inc=1, device_id={"tp": dev}, device_id_type=MESH)
        pl.semaphore_wait(barrier, 3)

    def ring_copy(buf, send, recv, half, hop, step, piece):
        blk = chip_at(half, hop) * 2 + core
        pieces = send.shape[2]
        size = buf.shape[2] // pieces
        ref = buf.at[half, blk, pl.ds(piece * size, size)]
        return remote(ref, ref, send.at[half, step, piece], recv.at[half, step, piece], next_dev(half))

    def pair_copy(buf, send, recv, half, hop):
        blk = chip_at(half, hop) * 2 + core
        return remote(buf.at[half, blk], buf.at[half, blk], send.at[half, hop], recv.at[half, hop], partner)

    def pair_arrival(buf, send, recv, half, hop):
        blk = chip_at(half, hop) * 2 + 1 - core
        return remote(buf.at[half, blk], buf.at[half, blk], send.at[half, hop], recv.at[half, hop], partner)

    def gather_begin(buf, sems, half):
        send, recv, psend_, precv_ = sems
        for piece in range(send.shape[2]):
            ring_copy(buf, send, recv, half, 0, 0, piece).start()
        pair_copy(buf, psend_, precv_, half, 0).start()

    def gather_step(buf, sems, step):
        send, recv, psend_, precv_ = sems
        for piece in range(send.shape[2]):
            for half in (0, 1):
                ring_copy(buf, send, recv, half, step + 1, step, piece).wait_recv()

                @pl.when(step + 1 < steps)
                def _():
                    ring_copy(buf, send, recv, half, step + 1, step + 1, piece).start()

        for half in (0, 1):
            pair_copy(buf, psend_, precv_, half, step + 1).start()

    def gather_drain(buf, sems):
        send, recv, psend_, precv_ = sems

        def body(step, _):
            for half in (0, 1):
                for piece in range(send.shape[2]):
                    ring_copy(buf, send, recv, half, step, step, piece).wait_send()
            return 0

        lax.fori_loop(0, steps, body, 0)

        def pair_body(hop, _):
            for half in (0, 1):
                pair_copy(buf, psend_, precv_, half, hop).wait_send()
            return 0

        lax.fori_loop(0, chips, pair_body, 0)

    d_sems = (d_send, d_recv, dp_send, dp_recv)
    n_sems = (n_send, n_recv, np_send, np_recv)
    e_sems = (e_send, e_recv, ep_send, ep_recv)

    tab_copy = remote(table_hbm, tab_in, tab_sem.at[0], tab_sem.at[1], partner)
    tab_copy.start()
    for half in (0, 1):
        rows = dout_ref[half * half_rows:(half + 1) * half_rows, :].astype(F32)
        d_all[half, me] = rows.T.astype(BF16)
        gather_begin(d_all, d_sems, half)
    conv = 32

    def convert(src, start):
        def body(i, _):
            at = pl.multiple_of(i * conv, conv)
            dst = pl.multiple_of(start + i * conv, conv)
            tab_f32[pl.ds(dst, conv), :] = src[pl.ds(at, conv), :].astype(F32)
            return 0

        lax.fori_loop(0, shard_rows // conv, body, 0)

    tab_load.wait()
    with jax.named_scope("s_table"):
        convert(table_ref, core * shard_rows)
        tab_f32[pl.ds(2 * shard_rows, 8), :] = jnp.zeros((8, dim), F32)
        gather_step(d_all, d_sems, 0)
        tab_copy.wait()
        convert(tab_in, (1 - core) * shard_rows)
        gather_step(d_all, d_sems, 1)

    pieces = x_send.shape[2]
    size = half_rows // pieces

    def x_copy(half, step, piece):
        rows = pl.ds(piece * size, size)
        return remote(xs.at[half, step, rows], xs.at[half, step + 1, rows], x_send.at[half, step, piece],
                      x_recv.at[half, step, piece], next_dev(half))

    unroll = 8
    chip_base = chip * (2 * shard_rows)
    none = jnp.uint32(2 * shard_rows)

    def look_step(step, _):
        with jax.named_scope("s_look"):
            for half in (0, 1):
                base = ((chip_at(half, step + 1) * 2 + core) * 2 + half) * half_rows

                def rows_body(i, _):
                    at = i * unroll
                    for j in range(unroll):
                        row = (ids_ref[base + at + j] - chip_base).astype(jnp.uint32)
                        row = jnp.minimum(row, none).astype(jnp.int32)
                        gath[half, pl.ds(at + j, 1), :] = tab_f32[pl.ds(row, 1), :]
                    return 0

                lax.fori_loop(0, half_rows // unroll, rows_body, 0)

        with jax.named_scope("s_xsum"):
            for piece in range(pieces):
                rows = slice(piece * size, (piece + 1) * size)
                for half in (0, 1):
                    @pl.when(step == 0)
                    def _():
                        xs[half, step, rows] = gath[half, rows].astype(BF16)

                    @pl.when(step > 0)
                    def _():
                        x_copy(half, step - 1, piece).wait_recv()
                        xs[half, step, rows] = (gath[half, rows] + xs[half, step, rows].astype(F32)).astype(BF16)

                    @pl.when(step < steps)
                    def _():
                        x_copy(half, step, piece).start()

        @pl.when(step + 2 < steps)
        def _():
            with jax.named_scope("s_dstep"):
                gather_step(d_all, d_sems, step + 2)

        @pl.when(step == 0)
        def _():
            with jax.named_scope("s_setup"):
                setup()

        return 0

    def setup():
        dw1t_ref[...] = jnp.zeros(dw1t_ref.shape, F32)
        dw2_ref[...] = jnp.zeros(dw2_ref.shape, F32)
        w1_ref[...] = w1t_ref[...].astype(F32).T.astype(BF16)
        w2t_ref[...] = w2_ref[...].astype(F32).T.astype(BF16)
        gain_t[...] = jnp.broadcast_to(gain_ref[...].astype(F32), (dim, dim)).T
        rel = ids_vec[...] - me * shard_rows
        owned = ((rel >= 0) & (rel < shard_rows)).astype(F32).astype(BF16)
        nt = (((1,), (1,)), ((), ()))
        ones = jnp.ones((8, ids_vec.shape[1]), BF16)
        counts = lax.dot_general(ones, owned, nt, preferred_element_type=F32).astype(jnp.int32)
        count_ref[...] = (counts + (BUNCH - 1)) // BUNCH

    groups = ids_vec.shape[0]
    width = ids_vec.shape[1]
    tokens = groups * width
    batch = 8
    turns = groups // batch
    per_step = -(-turns // steps)

    def owned_lists(step):
        lane = lax.broadcasted_iota(jnp.int32, (batch, width), 1)
        sub8 = lax.broadcasted_iota(jnp.int32, (8, width), 0)
        before = (lax.broadcasted_iota(jnp.int32, (width, width), 0)
                  < lax.broadcasted_iota(jnp.int32, (width, width), 1)).astype(F32).astype(BF16)
        place = lax.broadcasted_iota(jnp.int32, (width, width), 0)
        nt = (((1,), (1,)), ((), ()))

        def turn(t, _):
            at = pl.multiple_of(t * batch, batch)
            rel = ids_vec[pl.ds(at, batch), :] - me * shard_rows
            owned = (rel >= 0) & (rel < shard_rows)
            rank = jnp.dot(owned.astype(F32).astype(BF16), before, preferred_element_type=F32).astype(jnp.int32)
            rank = jnp.where(owned, rank, -1)
            rel = jnp.where(owned, rel, 0)
            count = jnp.sum(owned.astype(F32), axis=1, keepdims=True).astype(jnp.int32)
            lines = []
            for g in range(batch):
                hot = (jnp.broadcast_to(rank[g:g + 1], (width, width)) == place).astype(F32).astype(BF16)
                row = jnp.broadcast_to(rel[g:g + 1], (8, width))
                vals = jnp.where(sub8 == 0, lane[:8], jnp.where(sub8 == 1, row // width, row % width))
                got = lax.dot_general(vals.astype(F32).astype(BF16), hot, nt, preferred_element_type=F32)
                got = got.astype(jnp.int32)
                start = (t * batch + g) * width
                place_0 = (((start // half_rows) % 2) * (tokens // 2) + (start // (2 * half_rows)) * half_rows
                           + start % half_rows)
                line = (got[1:2] * width + got[2:3]) * tokens + (got[0:1] + place_0)
                lines.append(jnp.where(lane[:1] < count[g:g + 1], line, shard_rows * tokens))
            list_ref[pl.ds(at, batch), :] = jnp.concatenate(lines, axis=0)
            return 0

        first = jnp.minimum((step - 1) * per_step, turns)
        last = jnp.minimum(step * per_step, turns)
        lax.fori_loop(first, last, turn, 0)

    lax.fori_loop(0, chips, look_step, 0)

    gain = jnp.concatenate([gain_t[...]] * (half_rows // dim), axis=1)
    with jax.named_scope("s_norm"):
        for half in (0, 1):
            rows_t = xs[half, steps].astype(F32).T
            inv = lax.rsqrt(jnp.mean(rows_t * rows_t, axis=0, keepdims=True) + NORM_EPS)
            x_t[half] = rows_t
            inv_r[half] = inv
            n_all[half, me] = (rows_t * inv * gain).astype(BF16)
            gather_begin(n_all, n_sems, half)

    def d_wait(hop, _):
        for half in (0, 1):
            pair_arrival(d_all, dp_send, dp_recv, half, hop).wait_recv()
        return 0

    with jax.named_scope("s_dwait"):
        lax.fori_loop(0, chips, d_wait, 0)

    nt = (((1,), (1,)), ((), ()))

    def mlp(half, blk, dst):
        sub = half_rows // 2
        left, right = slice(0, sub), slice(sub, 2 * sub)

        def front(lo, hi, cols, h_buf, du_buf):
            u = jnp.dot(w1t_ref[lo:hi], n_all[half, blk, :, cols], preferred_element_type=F32).astype(BF16).astype(F32)
            dh = jnp.dot(w2_ref[lo:hi], d_all[half, blk, :, cols], preferred_element_type=F32)
            sq = (GELU_C * GELU_A) * (u * u)
            th = jnp.tanh(u * (GELU_C + sq))
            sg = 0.5 + 0.5 * th
            h = u * sg
            slope = sg + (h * (1.0 - th)) * (GELU_C + 3.0 * sq)
            h_buf[lo:hi] = h.astype(BF16)
            du_buf[lo:hi] = (dh * slope).astype(BF16)

        def weights(lo, hi, cols, h_buf, du_buf):
            n_t, d_t = n_all[half, blk, :, cols], d_all[half, blk, :, cols]
            dw2_ref[lo:hi] += lax.dot_general(h_buf[lo:hi], d_t, nt, preferred_element_type=F32)
            dw1t_ref[lo:hi] += lax.dot_general(du_buf[lo:hi], n_t, nt, preferred_element_type=F32)

        def back(cols, h_buf, du_buf):
            dst[0, :, cols] = jnp.dot(w2t_ref[...], h_buf[...], preferred_element_type=F32)
            dst[1, :, cols] = jnp.dot(w1_ref[...], du_buf[...], preferred_element_type=F32)

        for lo, hi in tiles:
            front(lo, hi, left, h_a, du_a)
        for lo, hi in tiles:
            weights(lo, hi, left, h_a, du_a)
            front(lo, hi, right, h_b, du_b)
        back(left, h_a, du_a)
        for lo, hi in tiles:
            weights(lo, hi, right, h_b, du_b)
        back(right, h_b, du_b)

    def order_of(half, hop):
        return (hop + half * (chips - 1)) % chips

    def p_copy(half, hop):
        return remote(parts.at[(order_of(half, hop) % 2) * 2 + half], precv.at[hop, half], p_send.at[hop, half],
                      p_recv.at[hop, half], partner)

    def r_copy(half, val, step):
        return remote(rs.at[step, half, val], rs.at[step + 1, half, val], r_send.at[step, half, val],
                      r_recv.at[step, half, val], next_dev(half))

    def part(g, _):
        turn = jnp.maximum(g - 1, 0)
        own_chip = jnp.where((g == 0) | (turn >= 4 * steps), 1, 0)
        late = turn - 4 * steps
        step = jnp.where(own_chip == 1, steps, turn // 4)
        half = jnp.where(own_chip == 1, jnp.where((late == 0) | (late == 2), 1, 0), (turn % 4) // 2)
        mine = jnp.where(own_chip == 1, jnp.where(late >= 1, 1, 0), turn % 2)
        hop = (step + 1) % chips
        blk = chip_at(half, hop) * 2 + (1 - core) * (1 - mine) + core * mine

        lead = min(3, steps)
        early = (g == 1) | ((g == 2) & (lead > 1)) | ((g == 4) & (lead > 2))
        steady = (turn % 4 == 0) & (turn >= 8) & (turn // 4 + 1 < steps)
        ahead = jnp.where(early, jnp.where(g == 4, 2, g - 1), turn // 4 + 1)

        @pl.when(early | steady)
        def _():
            with jax.named_scope("s_nstep"):
                gather_step(n_all, n_sems, ahead)

        @pl.when(mine == 0)
        def _():
            with jax.named_scope("s_npair"):
                pair_arrival(n_all, np_send, np_recv, half, hop).wait_recv()

            @pl.when(order_of(half, hop) >= 2)
            def _():
                p_copy(half, (hop + chips - 2) % chips).wait_send()

        spot = jnp.where(mine == 0, (order_of(half, hop) % 2) * 2 + half, 4)
        with jax.named_scope("s_mlp"):
            mlp(half, blk, parts.at[spot])

        @pl.when(mine == 0)
        def _():
            p_copy(half, hop).start()

        @pl.when(mine == 1)
        def _():
            with jax.named_scope("s_pwait"):
                p_copy(half, hop).wait_recv()
            for val in (1, 0):
                @pl.when(step == 0)
                def _():
                    rs[step, half, val] = parts[4, val] + precv[hop, half, val]

                @pl.when(step > 0)
                def _():
                    with jax.named_scope("s_rwait"):
                        r_copy(half, val, step - 1).wait_recv()
                    rs[step, half, val] = rs[step, half, val] + (parts[4, val] + precv[hop, half, val])

                @pl.when(step < steps)
                def _():
                    r_copy(half, val, step).start()

                if val == 1:
                    @pl.when(step == steps)
                    def _():
                        with jax.named_scope("s_fin"):
                            finish_dx(half)

            @pl.when((step < steps) & (half == 1))
            def _():
                with jax.named_scope("s_lists"):
                    owned_lists(step + 1)

        return 0

    def dx_put(half, blk):
        return pltpu.make_async_copy(dx_all.at[half, blk], dx_hbm.at[half, blk], dx_sem.at[half, blk])

    def finish_dx(half):
        gain = jnp.concatenate([gain_t[...]] * (half_rows // dim), axis=1)
        xv = x_t[half]
        inv = inv_r[half]
        rows = pl.ds(pl.multiple_of(half * half_rows, half_rows), half_rows)
        scaled = rs[steps, half, 1] * gain
        mean = jnp.mean(xv * scaled, axis=0, keepdims=True)
        dx = inv * (scaled - xv * inv * inv * mean)
        dx = dout_ref[rows, :].astype(F32) + dx.T
        dx_all[half, me] = dx.astype(BF16)
        gather_begin(dx_all, e_sems, half)
        dx_put(half, me).start()

    lax.fori_loop(0, 4 * chips, part, 0)

    puts = [
        pltpu.make_async_copy(src, dst, put_sem.at[i])
        for i, (src, dst) in enumerate((
            (dw1t_ref, dw1t_hbm), (dw2_ref, dw2_hbm), (list_ref, list_hbm), (count_ref, count_hbm), (out_ref, out_hbm),
        ))
    ]
    for put in puts[:4]:
        put.start()

    for half in (0, 1):
        rows = slice(half * half_rows, (half + 1) * half_rows)
        out_ref[rows, :] = (x_t[half] + rs[steps, half, 0]).T.astype(BF16)

    puts[4].start()

    def pair_done(hop):
        for half in (0, 1):
            pair_arrival(dx_all, ep_send, ep_recv, half, hop).wait_recv()
            dx_put(half, chip_at(half, hop) * 2 + 1 - core).start()

    def e_step(step, _):
        with jax.named_scope("s_estep"):
            gather_step(dx_all, e_sems, step)
        for half in (0, 1):
            dx_put(half, chip_at(half, step + 1) * 2 + core).start()
        pair_done(step)
        return 0

    lax.fori_loop(0, steps, e_step, 0)

    for buf, sems in ((d_all, d_sems), (n_all, n_sems)):
        gather_drain(buf, sems)

    def drain(step, _):
        for half in (0, 1):
            for piece in range(pieces):
                x_copy(half, step, piece).wait_send()
            for val in (0, 1):
                r_copy(half, val, step).wait_send()
        return 0

    lax.fori_loop(0, steps, drain, 0)
    for half in (0, 1):
        for order in (chips - 2, chips - 1):
            p_copy(half, (order + half) % chips).wait_send()
    for put in puts:
        put.wait()
    pair_done(steps)
    with jax.named_scope("s_edrain"):
        gather_drain(dx_all, e_sems)

    def put_wait(blk, _):
        for half in (0, 1):
            dx_put(half, blk).wait()
        return 0

    lax.fori_loop(0, 2 * chips, put_wait, 0)


def row_tiles(hidden):
    count = 4 if hidden >= 512 else 1
    cut = -(-hidden // (16 * count)) * 16
    edges = [min(i * cut, hidden) for i in range(count)] + [hidden]
    return tuple(zip(edges[:-1], edges[1:]))


def run_block(chips, ids, table, gain, w_up, w_down, d_out):
    rows, dim = d_out.shape
    shard_rows = table.shape[0]
    hidden = w_down.shape[0]
    half = rows // 2
    devs = 2 * chips
    sub = half // 2
    dma = pltpu.SemaphoreType.DMA
    vmem = pl.BlockSpec(memory_space=pltpu.VMEM)
    tokens = rows * devs
    groups = tokens // dim

    def gather_sems(pieces):
        ring, pair = (2, chips - 1, pieces), (2, chips)
        return [dma(ring), dma(ring), dma(pair), dma(pair)]

    results = (
        jax.ShapeDtypeStruct((rows, dim), BF16),
        jax.ShapeDtypeStruct((hidden, dim), F32),
        jax.ShapeDtypeStruct((hidden, dim), F32),
        jax.ShapeDtypeStruct((2, devs, half, dim), BF16),
        jax.ShapeDtypeStruct((groups, dim), jnp.int32),
        jax.ShapeDtypeStruct((8, groups), jnp.int32),
    )
    hbm = pl.BlockSpec(memory_space=pltpu.HBM)
    return pl.pallas_call(
        functools.partial(block_kernel, chips, row_tiles(hidden)),
        out_shape=results,
        in_specs=[pl.BlockSpec(memory_space=pltpu.SMEM), vmem, hbm] + [vmem] * 4,
        out_specs=(hbm,) * 6,
        scratch_shapes=[
            *[pltpu.VMEM(r.shape, r.dtype) for r in results],
            pltpu.VMEM((shard_rows, dim), BF16),
            pltpu.VMEM((shard_rows, dim), BF16),
            pltpu.VMEM((2 * shard_rows + 8, dim), F32),
            pltpu.VMEM((2, half, dim), F32),
            pltpu.VMEM((2, chips, half, dim), BF16),
            pltpu.VMEM((2, dim, half), F32),
            pltpu.VMEM((2, 1, half), F32),
            pltpu.VMEM((dim, dim), F32),
            pltpu.VMEM((dim, hidden), BF16),
            pltpu.VMEM((dim, hidden), BF16),
            pltpu.VMEM((2, devs, dim, half), BF16),
            pltpu.VMEM((2, devs, dim, half), BF16),
            *[pltpu.VMEM((hidden, sub), BF16)] * 4,
            pltpu.VMEM((5, 2, dim, half), F32),
            pltpu.VMEM((chips, 2, 2, dim, half), F32),
            pltpu.VMEM((chips, 2, 2, dim, half), F32),
            dma((3,)), dma((5,)), dma((2, devs)),
            dma((2, chips - 1, 2)), dma((2, chips - 1, 2)),
            *gather_sems(2), *gather_sems(4), *gather_sems(4),
            dma((chips, 2)), dma((chips, 2)),
            dma((chips - 1, 2, 2)), dma((chips - 1, 2, 2)),
        ],
        compiler_params=pltpu.CompilerParams(
            collective_id=0, has_side_effects=True, vmem_limit_bytes=67043328,
        ),
        cost_estimate=pl.CostEstimate(flops=12 * tokens * hidden * dim, bytes_accessed=tokens * dim * 8,
                                      transcendentals=0),
        name="block",
    )(ids, ids.reshape(groups, dim), table, gain.reshape(1, dim), w_up.T, w_down, d_out)


def scatter_kernel(extra, list_hbm, count_hbm, dx_ref, *refs):
    extra_in, grad_ref, extra_out = refs[:extra], refs[extra], refs[extra + 1:2 * extra + 1]
    acc, acc_odd, dx_in, dx_f32, list_ref, count_ref, in_sem, ex_sem, small_sem = refs[2 * extra + 1:2 * extra + 10]
    extra_buf = refs[2 * extra + 10:]
    blocks, block = dx_in.shape[:2]
    groups = list_ref.shape[0]
    tokens = dx_f32.shape[0]
    shard_rows = grad_ref.shape[0]
    shift = tokens.bit_length() - 1

    def load(b):
        return pltpu.make_async_copy(dx_ref.at[pl.ds(b * block, block)], dx_in.at[b], in_sem.at[b])

    def take(e):
        return pltpu.make_async_copy(extra_in[e], extra_buf[e], ex_sem.at[0, e])

    def give(e):
        return pltpu.make_async_copy(extra_buf[e], extra_out[e], ex_sem.at[1, e])

    small = (
        pltpu.make_async_copy(list_hbm, list_ref, small_sem.at[0]),
        pltpu.make_async_copy(count_hbm, count_ref, small_sem.at[1]),
    )
    for copy in small:
        copy.start()
    for b in range(blocks):
        load(b).start()
    for e in range(extra):
        take(e).start()
    acc[...] = jnp.zeros(acc.shape, F32)
    acc_odd[...] = jnp.zeros(acc.shape, F32)
    conv = 128

    for b in range(blocks):
        load(b).wait()

        def convert(i, _):
            at = pl.multiple_of(i * conv, conv)
            dst = pl.multiple_of(b * block + i * conv, conv)
            dx_f32[pl.ds(dst, conv), :] = dx_in[b, pl.ds(at, conv), :].astype(F32)
            return 0

        lax.fori_loop(0, block // conv, convert, 0)
    for e in range(extra):
        take(e).wait()
        give(e).start()
    for copy in small:
        copy.wait()

    def group(g, _):
        def bunch(i, _):
            for j in range(BUNCH):
                packed = list_ref[g, i * BUNCH + j]
                into = acc_odd if j % 2 else acc
                into[pl.ds(packed >> shift, 1), :] += dx_f32[pl.ds(packed & (tokens - 1), 1), :]
            return 0

        lax.fori_loop(0, count_ref[0, g], bunch, 0)
        return 0

    with jax.named_scope("s_rows"):
        lax.fori_loop(0, groups, group, 0)
    cut = -(-shard_rows // (8 * blocks)) * 8

    def flush(b):
        rows = pl.ds(b * cut, min(cut, shard_rows - b * cut))
        return pltpu.make_async_copy(acc.at[rows], grad_ref.at[rows], in_sem.at[b])

    used = [b for b in range(blocks) if b * cut < shard_rows]
    for b in used:
        rows = slice(b * cut, min((b + 1) * cut, shard_rows))
        acc[rows] = acc[rows] + acc_odd[rows]
        flush(b).start()
    for e in range(extra):
        give(e).wait()
    for b in used:
        flush(b).wait()


def scatter_rows(shard_rows, lists, counts, dx_all, others):
    tokens, dim = dx_all.shape
    hbm = pl.BlockSpec(memory_space=pltpu.HBM)
    blocks = 8
    extra = len(others)
    shapes = [jax.ShapeDtypeStruct((shard_rows, dim), F32)] + [jax.ShapeDtypeStruct(o.shape, o.dtype) for o in others]
    return pl.pallas_call(
        functools.partial(scatter_kernel, extra),
        out_shape=tuple(shapes),
        in_specs=[hbm] * (3 + extra),
        out_specs=(hbm,) * (1 + extra),
        scratch_shapes=[
            pltpu.VMEM((shard_rows + 8, dim), F32),
            pltpu.VMEM((shard_rows + 8, dim), F32),
            pltpu.VMEM((blocks, tokens // blocks, dim), BF16),
            pltpu.VMEM((tokens, dim), F32),
            pltpu.SMEM(lists.shape, jnp.int32),
            pltpu.SMEM(counts.shape, jnp.int32),
            pltpu.SemaphoreType.DMA((blocks,)),
            pltpu.SemaphoreType.DMA((2, extra)),
            pltpu.SemaphoreType.DMA((2,)),
            *[pltpu.VMEM(o.shape, o.dtype) for o in others],
        ],
        compiler_params=pltpu.CompilerParams(vmem_limit_bytes=67043328),
        name="scatter",
    )(lists, counts, dx_all, *others)


def solution(mesh):
    chips = mesh.shape["tp"] // 2

    def shard_body(token_ids, embed_table, norm_gain, w_up, w_down, d_out):
        shard_rows, dim = embed_table.shape
        block_out, dw1t, dw2, dx_all, lists, counts = run_block(
            chips, token_ids, embed_table, norm_gain, w_up, w_down, d_out)
        grad_table, block_out, dw1t, dw2 = scatter_rows(
            shard_rows, lists, counts, dx_all.reshape(-1, dim), (block_out, dw1t, dw2))
        return block_out, grad_table, dw1t.T, dw2

    return jax.shard_map(
        shard_body,
        mesh=mesh,
        in_specs=(P("dp"), P("tp", None), P(), P(None, "tp"), P("tp", None), P(("dp", "tp"), None)),
        out_specs=(P(("dp", "tp"), None), P(("dp", "tp"), None), P("dp", "tp"), P(("dp", "tp"), None)),
        check_vma=False,
    )
```

```python
import functools

import jax
import jax.numpy as jnp
from jax import lax
from jax.experimental import pallas as pl
from jax.experimental.pallas import tpu as pltpu
from jax.sharding import PartitionSpec as P

NORM_EPS = 1e-6
GELU_C = 0.7978845608028654
GELU_A = 0.044715
BUNCH = 4
MESH = pl.DeviceIdType.MESH
F32 = jnp.float32
BF16 = jnp.bfloat16


def remote(src, dst, send_sem, recv_sem, dev):
    return pltpu.make_async_remote_copy(
        src_ref=src, dst_ref=dst, send_sem=send_sem, recv_sem=recv_sem,
        device_id={"tp": dev}, device_id_type=MESH,
    )


def block_kernel(
    chips, tiles,
    ids_ref, ids_vec, table_hbm, gain_ref, w1t_ref, w2_ref, dout_ref,
    out_hbm, dw1t_hbm, dw2_hbm, dx_hbm, list_hbm, count_hbm,
    out_ref, dw1t_ref, dw2_ref, dx_all, list_ref, count_ref,
    table_ref, tab_in, tab_f32, gath, xs, x_t, inv_r, gain_t, w1_ref, w2t_ref, d_all, n_all,
    h_a, h_b, du_a, du_b, parts, precv, rs,
    tab_sem, put_sem, dx_sem, x_send, x_recv, d_send, d_recv, dp_recv, n_send, n_recv, np_recv,
    e_send, e_recv, ep_recv, p_send, p_recv, r_send, r_recv,
):
    me = lax.axis_index("tp")
    chip, core = me // 2, me % 2
    partner = chip * 2 + 1 - core
    up = ((chip + 1) % chips) * 2 + core
    down = ((chip + chips - 1) % chips) * 2 + core
    half_rows, dim = gath.shape[1:]
    shard_rows = table_ref.shape[0]
    steps = chips - 1

    def next_dev(half):
        return up * (1 - half) + down * half

    def chip_at(half, hop):
        return (chip + (1 - half) * (chips - hop) + half * hop) % chips

    tab_load = pltpu.make_async_copy(table_hbm, table_ref, tab_sem.at[2])
    tab_load.start()
    barrier = pltpu.get_barrier_semaphore()
    for dev in (partner, up, down):
        pl.semaphore_signal(barrier, inc=1, device_id={"tp": dev}, device_id_type=MESH)
    pl.semaphore_wait(barrier, 3)

    def ring_copy(buf, send, recv, half, hop, step, piece):
        blk = chip_at(half, hop) * 2 + core
        size = buf.shape[2] // recv.shape[2]
        ref = buf.at[half, blk, pl.ds(piece * size, size)]
        return remote(ref, ref, send.at[0], recv.at[half, step, piece], next_dev(half))

    def pair_copy(buf, send, recv, half, hop):
        blk = chip_at(half, hop) * 2 + core
        return remote(buf.at[half, blk], buf.at[half, blk], send.at[1], recv.at[half, hop], partner)

    def pair_arrival(buf, send, recv, half, hop):
        blk = chip_at(half, hop) * 2 + 1 - core
        return remote(buf.at[half, blk], buf.at[half, blk], send.at[1], recv.at[half, hop], partner)

    def gather_begin(buf, sems, half):
        send, recv, pair_recv = sems
        for piece in range(recv.shape[2]):
            ring_copy(buf, send, recv, half, 0, 0, piece).start()
        pair_copy(buf, send, pair_recv, half, 0).start()

    def gather_step(buf, sems, step):
        send, recv, pair_recv = sems
        for piece in range(recv.shape[2]):
            for half in (0, 1):
                ring_copy(buf, send, recv, half, step + 1, step, piece).wait_recv()

                @pl.when(step + 1 < steps)
                def _():
                    ring_copy(buf, send, recv, half, step + 1, step + 1, piece).start()

        for half in (0, 1):
            pair_copy(buf, send, pair_recv, half, step + 1).start()

    def gather_drain(buf, sems):
        send, recv, pair_recv = sems
        ring = buf.at[:, pl.ds(0, steps)]
        pair = buf.at[:, pl.ds(0, chips)]
        remote(ring, ring, send.at[0], recv.at[0, 0, 0], partner).wait_send()
        remote(pair, pair, send.at[1], pair_recv.at[0, 0], partner).wait_send()

    d_sems = (d_send, d_recv, dp_recv)
    n_sems = (n_send, n_recv, np_recv)
    e_sems = (e_send, e_recv, ep_recv)

    tab_copy = remote(table_hbm, tab_in, tab_sem.at[0], tab_sem.at[1], partner)
    tab_copy.start()
    for half in (0, 1):
        rows = dout_ref[half * half_rows:(half + 1) * half_rows, :].astype(F32)
        d_all[half, me] = rows.T.astype(BF16)
        gather_begin(d_all, d_sems, half)
    conv = 32

    def convert(src, start):
        def body(i, _):
            at = pl.multiple_of(i * conv, conv)
            dst = pl.multiple_of(start + i * conv, conv)
            tab_f32[pl.ds(dst, conv), :] = src[pl.ds(at, conv), :].astype(F32)
            return 0

        lax.fori_loop(0, shard_rows // conv, body, 0)

    tab_load.wait()
    convert(table_ref, core * shard_rows)
    tab_f32[pl.ds(2 * shard_rows, 8), :] = jnp.zeros((8, dim), F32)
    tab_copy.wait()
    convert(tab_in, (1 - core) * shard_rows)
    tail = max(steps - 3, 0)
    if tail > 0:
        gather_step(d_all, d_sems, 0)

    pieces = x_recv.shape[2]
    size = half_rows // pieces

    def x_copy(half, step, piece):
        rows = pl.ds(piece * size, size)
        return remote(xs.at[half, step, rows], xs.at[half, step + 1, rows], x_send.at[0],
                      x_recv.at[half, step, piece], next_dev(half))

    unroll = 8
    chip_base = chip * (2 * shard_rows)
    none = jnp.uint32(2 * shard_rows)

    def look_step(step, _):
        for half in (0, 1):
            base = ((chip_at(half, step + 1) * 2 + core) * 2 + half) * half_rows

            def rows_body(i, _):
                at = i * unroll
                for j in range(unroll):
                    row = (ids_ref[base + at + j] - chip_base).astype(jnp.uint32)
                    row = jnp.minimum(row, none).astype(jnp.int32)
                    gath[half, pl.ds(at + j, 1), :] = tab_f32[pl.ds(row, 1), :]
                return 0

            lax.fori_loop(0, half_rows // unroll, rows_body, 0)

        for piece in range(pieces):
            rows = slice(piece * size, (piece + 1) * size)
            for half in (0, 1):
                @pl.when(step == 0)
                def _():
                    xs[half, step, rows] = gath[half, rows].astype(BF16)

                @pl.when(step > 0)
                def _():
                    x_copy(half, step - 1, piece).wait_recv()
                    xs[half, step, rows] = (gath[half, rows] + xs[half, step, rows].astype(F32)).astype(BF16)

                @pl.when(step < steps)
                def _():
                    x_copy(half, step, piece).start()

        @pl.when(step + 1 < tail)
        def _():
            gather_step(d_all, d_sems, step + 1)

        @pl.when(step == 0)
        def _():
            setup()

        return 0

    def setup():
        dw1t_ref[...] = jnp.zeros(dw1t_ref.shape, F32)
        dw2_ref[...] = jnp.zeros(dw2_ref.shape, F32)
        w1_ref[...] = w1t_ref[...].astype(F32).T.astype(BF16)
        w2t_ref[...] = w2_ref[...].astype(F32).T.astype(BF16)
        gain_t[...] = jnp.broadcast_to(gain_ref[...].astype(F32), (dim, dim)).T
        rel = ids_vec[...] - me * shard_rows
        owned = ((rel >= 0) & (rel < shard_rows)).astype(F32).astype(BF16)
        nt = (((1,), (1,)), ((), ()))
        ones = jnp.ones((8, ids_vec.shape[1]), BF16)
        counts = lax.dot_general(ones, owned, nt, preferred_element_type=F32).astype(jnp.int32)
        count_ref[...] = (counts + (BUNCH - 1)) // BUNCH

    groups = ids_vec.shape[0]
    width = ids_vec.shape[1]
    tokens = groups * width
    batch = 8
    turns = groups // batch
    per_step = -(-turns // steps)

    def owned_lists(step):
        lane = lax.broadcasted_iota(jnp.int32, (batch, width), 1)
        sub8 = lax.broadcasted_iota(jnp.int32, (8, width), 0)
        before = (lax.broadcasted_iota(jnp.int32, (width, width), 0)
                  < lax.broadcasted_iota(jnp.int32, (width, width), 1)).astype(F32).astype(BF16)
        place = lax.broadcasted_iota(jnp.int32, (width, width), 0)
        nt = (((1,), (1,)), ((), ()))

        def turn(t, _):
            at = pl.multiple_of(t * batch, batch)
            rel = ids_vec[pl.ds(at, batch), :] - me * shard_rows
            owned = (rel >= 0) & (rel < shard_rows)
            rank = jnp.dot(owned.astype(F32).astype(BF16), before, preferred_element_type=F32).astype(jnp.int32)
            rank = jnp.where(owned, rank, -1)
            rel = jnp.where(owned, rel, 0)
            count = jnp.sum(owned.astype(F32), axis=1, keepdims=True).astype(jnp.int32)
            lines = []
            for g in range(batch):
                hot = (jnp.broadcast_to(rank[g:g + 1], (width, width)) == place).astype(F32).astype(BF16)
                row = jnp.broadcast_to(rel[g:g + 1], (8, width))
                vals = jnp.where(sub8 == 0, lane[:8], jnp.where(sub8 == 1, row // width, row % width))
                got = lax.dot_general(vals.astype(F32).astype(BF16), hot, nt, preferred_element_type=F32)
                got = got.astype(jnp.int32)
                start = (t * batch + g) * width
                place_0 = (((start // half_rows) % 2) * (tokens // 2) + (start // (2 * half_rows)) * half_rows
                           + start % half_rows)
                line = (got[1:2] * width + got[2:3]) * tokens + (got[0:1] + place_0)
                lines.append(jnp.where(lane[:1] < count[g:g + 1], line, shard_rows * tokens))
            list_ref[pl.ds(at, batch), :] = jnp.concatenate(lines, axis=0)
            return 0

        first = jnp.minimum((step - 1) * per_step, turns)
        last = jnp.minimum(step * per_step, turns)
        lax.fori_loop(first, last, turn, 0)

    lax.fori_loop(0, chips, look_step, 0)

    gain = jnp.concatenate([gain_t[...]] * (half_rows // dim), axis=1)
    for half in (0, 1):
        rows_t = xs[half, steps].astype(F32).T
        inv = lax.rsqrt(jnp.mean(rows_t * rows_t, axis=0, keepdims=True) + NORM_EPS)
        x_t[half] = rows_t
        inv_r[half] = inv
        n_all[half, me] = (rows_t * inv * gain).astype(BF16)
        gather_begin(n_all, n_sems, half)

    nt = (((1,), (1,)), ((), ()))

    def mlp(half, blk, dst):
        sub = half_rows // 2
        left, right = slice(0, sub), slice(sub, 2 * sub)

        def front(lo, hi, cols, h_buf, du_buf):
            u = jnp.dot(w1t_ref[lo:hi], n_all[half, blk, :, cols], preferred_element_type=F32).astype(BF16).astype(F32)
            dh = jnp.dot(w2_ref[lo:hi], d_all[half, blk, :, cols], preferred_element_type=F32)
            sq = (GELU_C * GELU_A) * (u * u)
            th = jnp.tanh(u * (GELU_C + sq))
            sg = 0.5 + 0.5 * th
            h = u * sg
            slope = sg + (h * (1.0 - th)) * (GELU_C + 3.0 * sq)
            h_buf[lo:hi] = h.astype(BF16)
            du_buf[lo:hi] = (dh * slope).astype(BF16)

        def weights(lo, hi, cols, h_buf, du_buf):
            n_t, d_t = n_all[half, blk, :, cols], d_all[half, blk, :, cols]
            dw2_ref[lo:hi] += lax.dot_general(h_buf[lo:hi], d_t, nt, preferred_element_type=F32)
            dw1t_ref[lo:hi] += lax.dot_general(du_buf[lo:hi], n_t, nt, preferred_element_type=F32)

        def back(cols, h_buf, du_buf):
            dst[0, :, cols] = jnp.dot(w2t_ref[...], h_buf[...], preferred_element_type=F32)
            dst[1, :, cols] = jnp.dot(w1_ref[...], du_buf[...], preferred_element_type=F32)

        for lo, hi in tiles:
            front(lo, hi, left, h_a, du_a)
        for lo, hi in tiles:
            weights(lo, hi, left, h_a, du_a)
            front(lo, hi, right, h_b, du_b)
        back(left, h_a, du_a)
        for lo, hi in tiles:
            weights(lo, hi, right, h_b, du_b)
        back(right, h_b, du_b)

    def order_of(half, hop):
        return (hop + half * (chips - 1)) % chips

    def p_copy(half, hop):
        return remote(parts.at[(order_of(half, hop) % 2) * 2 + half], precv.at[hop, half], p_send.at[hop, half],
                      p_recv.at[hop, half], partner)

    def r_copy(half, val, step):
        return remote(rs.at[step, half, val], rs.at[step + 1, half, val], r_send.at[0],
                      r_recv.at[step, half, val], next_dev(half))

    def part(g, _):
        turn = jnp.maximum(g - 1, 0)
        own_chip = jnp.where((g == 0) | (turn >= 4 * steps), 1, 0)
        late = turn - 4 * steps
        step = jnp.where(own_chip == 1, steps, turn // 4)
        half = jnp.where(own_chip == 1, jnp.where((late == 0) | (late == 2), 1, 0), (turn % 4) // 2)
        mine = jnp.where(own_chip == 1, jnp.where(late >= 1, 1, 0), turn % 2)
        hop = (step + 1) % chips
        blk = chip_at(half, hop) * 2 + (1 - core) * (1 - mine) + core * mine

        lead = min(3, steps)
        early = (g == 1) | ((g == 2) & (lead > 1)) | ((g == 4) & (lead > 2))
        steady = (turn % 4 == 0) & (turn >= 8) & (turn // 4 + 1 < steps)
        ahead = jnp.where(early, jnp.where(g == 4, 2, g - 1), turn // 4 + 1)

        @pl.when(early | steady)
        def _():
            gather_step(n_all, n_sems, ahead)

        @pl.when((g <= 1) | (g == 5))
        def _():
            gather_step(d_all, d_sems, tail + jnp.where(g == 5, 2, g))

        @pl.when(mine == 0)
        def _():
            pair_arrival(n_all, n_send, np_recv, half, hop).wait_recv()
            pair_arrival(d_all, d_send, dp_recv, half, hop).wait_recv()

            @pl.when(order_of(half, hop) >= 2)
            def _():
                p_copy(half, (hop + chips - 2) % chips).wait_send()

        spot = jnp.where(mine == 0, (order_of(half, hop) % 2) * 2 + half, 4 + half)
        mlp(half, blk, parts.at[spot])

        @pl.when(mine == 0)
        def _():
            p_copy(half, hop).start()

        @pl.when(mine == 1)
        def _():
            p_copy(half, hop).wait_recv()
            for val in (1, 0):
                @pl.when(step == 0)
                def _():
                    rs[step, half, val] = parts[4 + half, val] + precv[hop, half, val]

                @pl.when((step > 0) & ((step < steps) | (val == 1)))
                def _():
                    r_copy(half, val, step - 1).wait_recv()
                    rs[step, half, val] = rs[step, half, val] + (parts[4 + half, val] + precv[hop, half, val])

                @pl.when(step < steps)
                def _():
                    r_copy(half, val, step).start()

                if val == 1:
                    @pl.when(step == steps)
                    def _():
                        finish_dx(half)

            @pl.when((step < steps) & (half == 1))
            def _():
                owned_lists(step + 1)

        return 0

    def dx_put(half, blk):
        return pltpu.make_async_copy(dx_all.at[half, blk], dx_hbm.at[half, blk], dx_sem.at[0])

    def finish_dx(half):
        gain = jnp.concatenate([gain_t[...]] * (half_rows // dim), axis=1)
        xv = x_t[half]
        inv = inv_r[half]
        rows = pl.ds(pl.multiple_of(half * half_rows, half_rows), half_rows)
        scaled = rs[steps, half, 1] * gain
        mean = jnp.mean(xv * scaled, axis=0, keepdims=True)
        dx = inv * (scaled - xv * inv * inv * mean)
        dx = dout_ref[rows, :].astype(F32) + dx.T
        dx_all[half, me] = dx.astype(BF16)
        gather_begin(dx_all, e_sems, half)
        dx_put(half, me).start()

    lax.fori_loop(0, 4 * chips, part, 0)

    puts = [
        pltpu.make_async_copy(src, dst, put_sem.at[i])
        for i, (src, dst) in enumerate((
            (dw1t_ref, dw1t_hbm), (dw2_ref, dw2_hbm), (list_ref, list_hbm), (count_ref, count_hbm), (out_ref, out_hbm),
        ))
    ]
    for put in puts[:4]:
        put.start()

    def finish_out():
        for half in (0, 1):
            rows = slice(half * half_rows, (half + 1) * half_rows)
            r_copy(half, 0, steps - 1).wait_recv()
            y = rs[steps, half, 0] + (parts[4 + half, 0] + precv[0, half, 0])
            out_ref[rows, :] = (x_t[half] + y).T.astype(BF16)
        puts[4].start()

    def pair_done(hop):
        for half in (0, 1):
            pair_arrival(dx_all, e_send, ep_recv, half, hop).wait_recv()
            dx_put(half, chip_at(half, hop) * 2 + 1 - core).start()

    def e_step(step, _):
        gather_step(dx_all, e_sems, step)
        for half in (0, 1):
            dx_put(half, chip_at(half, step + 1) * 2 + core).start()
        pair_done(step)

        @pl.when(step == min(2, steps - 1))
        def _():
            finish_out()

        return 0

    lax.fori_loop(0, steps, e_step, 0)

    for buf, sems in ((d_all, d_sems), (n_all, n_sems)):
        gather_drain(buf, sems)

    sent = xs.at[:, pl.ds(0, steps)]
    remote(sent, sent, x_send.at[0], x_recv.at[0, 0, 0], partner).wait_send()
    sent = rs.at[pl.ds(0, steps)]
    remote(sent, sent, r_send.at[0], r_recv.at[0, 0, 0], partner).wait_send()
    for half in (0, 1):
        for order in (chips - 2, chips - 1):
            p_copy(half, (order + half) % chips).wait_send()
    for put in puts:
        put.wait()
    pair_done(steps)
    gather_drain(dx_all, e_sems)

    pltpu.make_async_copy(dx_all, dx_hbm, dx_sem.at[0]).wait()


def row_tiles(hidden):
    count = 4 if hidden >= 512 else 1
    cut = -(-hidden // (16 * count)) * 16
    edges = [min(i * cut, hidden) for i in range(count)] + [hidden]
    return tuple(zip(edges[:-1], edges[1:]))


def run_block(chips, ids, table, gain, w_up, w_down, d_out):
    rows, dim = d_out.shape
    shard_rows = table.shape[0]
    hidden = w_down.shape[0]
    half = rows // 2
    devs = 2 * chips
    sub = half // 2
    dma = pltpu.SemaphoreType.DMA
    vmem = pl.BlockSpec(memory_space=pltpu.VMEM)
    tokens = rows * devs
    groups = tokens // dim

    def gather_sems(pieces):
        return [dma((2,)), dma((2, chips - 1, pieces)), dma((2, chips))]

    results = (
        jax.ShapeDtypeStruct((rows, dim), BF16),
        jax.ShapeDtypeStruct((hidden, dim), F32),
        jax.ShapeDtypeStruct((hidden, dim), F32),
        jax.ShapeDtypeStruct((2, devs, half, dim), BF16),
        jax.ShapeDtypeStruct((groups, dim), jnp.int32),
        jax.ShapeDtypeStruct((8, groups), jnp.int32),
    )
    hbm = pl.BlockSpec(memory_space=pltpu.HBM)
    return pl.pallas_call(
        functools.partial(block_kernel, chips, row_tiles(hidden)),
        out_shape=results,
        in_specs=[pl.BlockSpec(memory_space=pltpu.SMEM), vmem, hbm] + [vmem] * 4,
        out_specs=(hbm,) * 6,
        scratch_shapes=[
            *[pltpu.VMEM(r.shape, r.dtype) for r in results],
            pltpu.VMEM((shard_rows, dim), BF16),
            pltpu.VMEM((shard_rows, dim), BF16),
            pltpu.VMEM((2 * shard_rows + 8, dim), F32),
            pltpu.VMEM((2, half, dim), F32),
            pltpu.VMEM((2, chips, half, dim), BF16),
            pltpu.VMEM((2, dim, half), F32),
            pltpu.VMEM((2, 1, half), F32),
            pltpu.VMEM((dim, dim), F32),
            pltpu.VMEM((dim, hidden), BF16),
            pltpu.VMEM((dim, hidden), BF16),
            pltpu.VMEM((2, devs, dim, half), BF16),
            pltpu.VMEM((2, devs, dim, half), BF16),
            *[pltpu.VMEM((hidden, sub), BF16)] * 4,
            pltpu.VMEM((6, 2, dim, half), F32),
            pltpu.VMEM((chips, 2, 2, dim, half), F32),
            pltpu.VMEM((chips, 2, 2, dim, half), F32),
            dma((3,)), dma((5,)), dma((1,)),
            dma((1,)), dma((2, chips - 1, 2)),
            *gather_sems(2), *gather_sems(2), *gather_sems(4),
            dma((chips, 2)), dma((chips, 2)),
            dma((1,)), dma((chips - 1, 2, 2)),
        ],
        compiler_params=pltpu.CompilerParams(
            collective_id=0, has_side_effects=True, vmem_limit_bytes=67043328,
        ),
        cost_estimate=pl.CostEstimate(flops=12 * tokens * hidden * dim, bytes_accessed=tokens * dim * 8,
                                      transcendentals=0),
        name="block",
    )(ids, ids.reshape(groups, dim), table, gain.reshape(1, dim), w_up.T, w_down, d_out)


def scatter_kernel(extra, list_hbm, count_hbm, dx_ref, *refs):
    extra_in, grad_ref, extra_out = refs[:extra], refs[extra], refs[extra + 1:2 * extra + 1]
    acc, acc_odd, dx_in, dx_f32, list_ref, count_ref, in_sem, ex_sem, small_sem = refs[2 * extra + 1:2 * extra + 10]
    extra_buf = refs[2 * extra + 10:]
    blocks, block = dx_in.shape[:2]
    groups = list_ref.shape[0]
    tokens = dx_f32.shape[0]
    shard_rows = grad_ref.shape[0]
    shift = tokens.bit_length() - 1

    def load(b):
        return pltpu.make_async_copy(dx_ref.at[pl.ds(b * block, block)], dx_in.at[b], in_sem.at[b])

    def take(e):
        return pltpu.make_async_copy(extra_in[e], extra_buf[e], ex_sem.at[0, e])

    def give(e):
        return pltpu.make_async_copy(extra_buf[e], extra_out[e], ex_sem.at[1, e])

    small = (
        pltpu.make_async_copy(list_hbm, list_ref, small_sem.at[0]),
        pltpu.make_async_copy(count_hbm, count_ref, small_sem.at[1]),
    )
    for copy in small:
        copy.start()
    for b in range(blocks):
        load(b).start()
    for e in range(extra):
        take(e).start()
    acc[...] = jnp.zeros(acc.shape, F32)
    acc_odd[...] = jnp.zeros(acc.shape, F32)
    conv = 128

    for b in range(blocks):
        load(b).wait()

        def convert(i, _):
            at = pl.multiple_of(i * conv, conv)
            dst = pl.multiple_of(b * block + i * conv, conv)
            dx_f32[pl.ds(dst, conv), :] = dx_in[b, pl.ds(at, conv), :].astype(F32)
            return 0

        lax.fori_loop(0, block // conv, convert, 0)
    for e in range(extra):
        take(e).wait()
        give(e).start()
    for copy in small:
        copy.wait()

    def group(g, _):
        def bunch(i, _):
            for j in range(BUNCH):
                packed = list_ref[g, i * BUNCH + j]
                into = acc_odd if j % 2 else acc
                into[pl.ds(packed >> shift, 1), :] += dx_f32[pl.ds(packed & (tokens - 1), 1), :]
            return 0

        lax.fori_loop(0, count_ref[0, g], bunch, 0)
        return 0

    lax.fori_loop(0, groups, group, 0)
    cut = -(-shard_rows // (8 * blocks)) * 8

    def flush(b):
        rows = pl.ds(b * cut, min(cut, shard_rows - b * cut))
        return pltpu.make_async_copy(acc.at[rows], grad_ref.at[rows], in_sem.at[b])

    used = [b for b in range(blocks) if b * cut < shard_rows]
    for b in used:
        rows = slice(b * cut, min((b + 1) * cut, shard_rows))
        acc[rows] = acc[rows] + acc_odd[rows]
        flush(b).start()
    for e in range(extra):
        give(e).wait()
    for b in used:
        flush(b).wait()


def scatter_rows(shard_rows, lists, counts, dx_all, others):
    tokens, dim = dx_all.shape
    hbm = pl.BlockSpec(memory_space=pltpu.HBM)
    blocks = 8
    extra = len(others)
    shapes = [jax.ShapeDtypeStruct((shard_rows, dim), F32)] + [jax.ShapeDtypeStruct(o.shape, o.dtype) for o in others]
    return pl.pallas_call(
        functools.partial(scatter_kernel, extra),
        out_shape=tuple(shapes),
        in_specs=[hbm] * (3 + extra),
        out_specs=(hbm,) * (1 + extra),
        scratch_shapes=[
            pltpu.VMEM((shard_rows + 8, dim), F32),
            pltpu.VMEM((shard_rows + 8, dim), F32),
            pltpu.VMEM((blocks, tokens // blocks, dim), BF16),
            pltpu.VMEM((tokens, dim), F32),
            pltpu.SMEM(lists.shape, jnp.int32),
            pltpu.SMEM(counts.shape, jnp.int32),
            pltpu.SemaphoreType.DMA((blocks,)),
            pltpu.SemaphoreType.DMA((2, extra)),
            pltpu.SemaphoreType.DMA((2,)),
            *[pltpu.VMEM(o.shape, o.dtype) for o in others],
        ],
        compiler_params=pltpu.CompilerParams(vmem_limit_bytes=67043328),
        name="scatter",
    )(lists, counts, dx_all, *others)


def solution(mesh):
    chips = mesh.shape["tp"] // 2

    def shard_body(token_ids, embed_table, norm_gain, w_up, w_down, d_out):
        shard_rows, dim = embed_table.shape
        block_out, dw1t, dw2, dx_all, lists, counts = run_block(
            chips, token_ids, embed_table, norm_gain, w_up, w_down, d_out)
        grad_table, block_out, dw1t, dw2 = scatter_rows(
            shard_rows, lists, counts, dx_all.reshape(-1, dim), (block_out, dw1t, dw2))
        return block_out, grad_table, dw1t.T, dw2

    return jax.shard_map(
        shard_body,
        mesh=mesh,
        in_specs=(P("dp"), P("tp", None), P(), P(None, "tp"), P("tp", None), P(("dp", "tp"), None)),
        out_specs=(P(("dp", "tp"), None), P(("dp", "tp"), None), P("dp", "tp"), P(("dp", "tp"), None)),
        check_vma=False,
    )
```
